32 devices in a mesh: dp: 1 (over z), tp: 4 (over y), sp: 8 (over x, core).
Axes of the slice: x: 4, y: 4, z: 1, core: 2. Of those that a mesh axis runs over, the one named last changes fastest.
The devices are a block of a 4x4x8 slice.
Arguments:
- hidden: bfloat16 [128, 4096], P('dp')
- seq_lens: int32 [128], P('dp')
- k_cache: bfloat16 [128, 8, 1024, 128], P('dp', 'tp', 'sp')
- v_cache: bfloat16 [128, 8, 1024, 128], P('dp', 'tp', 'sp')
- attn_norm: bfloat16 [4096], replicated
- w_q: bfloat16 [4096, 4096], P(None, 'tp')
- w_k: bfloat16 [4096, 1024], P(None, 'tp')
- w_v: bfloat16 [4096, 1024], P(None, 'tp')
- w_o: bfloat16 [4096, 4096], P('tp')
- mlp_norm: bfloat16 [4096], replicated
- w_gate: bfloat16 [4096, 14336], P(None, 'tp')
- w_up: bfloat16 [4096, 14336], P(None, 'tp')
- w_down: bfloat16 [14336, 4096], P('tp')
Outputs:
- output 1: bfloat16 [128, 4096], P('dp')
- output 2: bfloat16 [128, 8, 1024, 128], P('dp', 'tp', 'sp')
- output 3: bfloat16 [128, 8, 1024, 128], P('dp', 'tp', 'sp')
All inputs are finite; a program needn't handle non-finite values.
Results may differ from the reference program's by a relative error of at most 0.00515676.
Values sent between devices are 32-bit elements.
A program may use at most 768 MiB of HBM per device.

```python
import math
import jax
import jax.numpy as jnp
from jax import lax

BATCH = 128
SEQ = 1024
SEQ_BLOCK = 128
D = 4096
HEADS = 32
KV_HEADS = 8
HEAD = 128
FF = 14336

REP = HEADS // KV_HEADS
NORM_EPS = 1e-6


def draw_lens(key_long, key_tail):
    long_lens = jax.random.randint(key_long, (BATCH,), SEQ // 4, SEQ, dtype=jnp.int32)
    tail_lens = SEQ - 1 - jax.random.randint(key_tail, (BATCH,), 0, SEQ_BLOCK, dtype=jnp.int32)
    odd_rows = (jnp.arange(BATCH) % 2) == 1
    seq_lens = jnp.where(odd_rows, tail_lens, long_lens)
    return seq_lens.at[BATCH - 1].set(SEQ // 4).at[0].set(SEQ - 1)


def setup_inputs(seed: int = 0, part: int = 0) -> dict:
    part_key = jax.random.fold_in(jax.random.key(seed), part)
    key_hidden, key_kcache, key_vcache, key_long, key_tail = jax.random.split(part_key, 5)
    weight_keys = jax.random.split(jax.random.key(seed + 1), 9)
    hidden = jax.random.normal(key_hidden, (BATCH, D), jnp.float32)
    k_cache = jax.random.normal(key_kcache, (BATCH, KV_HEADS, SEQ, HEAD), jnp.float32)
    v_cache = jax.random.normal(key_vcache, (BATCH, KV_HEADS, SEQ, HEAD), jnp.float32)
    seq_lens = draw_lens(key_long, key_tail)
    attn_norm = 1.0 + 0.3 * jax.random.normal(weight_keys[0], (D,), jnp.float32)
    w_q = jax.random.normal(weight_keys[1], (D, HEADS * HEAD), jnp.float32) * D ** -0.5
    group_mean = jnp.mean(w_q.reshape(D, KV_HEADS, REP, HEAD), axis=2).reshape(D, KV_HEADS * HEAD)
    align = 0.5 * math.log(SEQ) * REP / math.sqrt(HEAD)
    w_k = align * group_mean + jax.random.normal(weight_keys[2], (D, KV_HEADS * HEAD), jnp.float32) * D ** -0.5
    w_v = jax.random.normal(weight_keys[3], (D, KV_HEADS * HEAD), jnp.float32) * D ** -0.5
    out_scale = 0.3 * math.sqrt(SEQ) / math.sqrt(HEADS * HEAD)
    w_o = jax.random.normal(weight_keys[4], (HEADS * HEAD, D), jnp.float32) * out_scale
    mlp_norm = 1.0 + 0.3 * jax.random.normal(weight_keys[5], (D,), jnp.float32)
    w_gate = jax.random.normal(weight_keys[6], (D, FF), jnp.float32) * D ** -0.5
    w_up = jax.random.normal(weight_keys[7], (D, FF), jnp.float32) * D ** -0.5
    w_down = jax.random.normal(weight_keys[8], (FF, D), jnp.float32) * FF ** -0.5
    return {
        'hidden': hidden.astype(jnp.bfloat16),
        'seq_lens': seq_lens,
        'k_cache': k_cache.astype(jnp.bfloat16),
        'v_cache': v_cache.astype(jnp.bfloat16),
        'attn_norm': attn_norm.astype(jnp.bfloat16),
        'w_q': w_q.astype(jnp.bfloat16),
        'w_k': w_k.astype(jnp.bfloat16),
        'w_v': w_v.astype(jnp.bfloat16),
        'w_o': w_o.astype(jnp.bfloat16),
        'mlp_norm': mlp_norm.astype(jnp.bfloat16),
        'w_gate': w_gate.astype(jnp.bfloat16),
        'w_up': w_up.astype(jnp.bfloat16),
        'w_down': w_down.astype(jnp.bfloat16),
    }


def rms_norm(values, gain):
    wide = values.astype(jnp.float32)
    scaled = wide * lax.rsqrt(jnp.mean(wide * wide, axis=-1, keepdims=True) + NORM_EPS)
    return (scaled * gain.astype(jnp.float32)).astype(jnp.bfloat16)


def reference(hidden, seq_lens, k_cache, v_cache, attn_norm, w_q, w_k, w_v, w_o, mlp_norm, w_gate, w_up, w_down):
    normed = rms_norm(hidden, attn_norm)
    query = jnp.dot(normed, w_q, preferred_element_type=jnp.float32).astype(jnp.bfloat16).reshape(BATCH, KV_HEADS, REP, HEAD)
    k_new = jnp.dot(normed, w_k, preferred_element_type=jnp.float32).astype(jnp.bfloat16).reshape(BATCH, KV_HEADS, 1, HEAD)
    v_new = jnp.dot(normed, w_v, preferred_element_type=jnp.float32).astype(jnp.bfloat16).reshape(BATCH, KV_HEADS, 1, HEAD)
    positions = jnp.arange(SEQ)
    new_slot = (positions[None, :] == seq_lens[:, None])[:, None, :, None]
    k_out = jnp.where(new_slot, k_new, k_cache)
    v_out = jnp.where(new_slot, v_new, v_cache)

    def attend(row):
        q_row, keys, values, length = row
        valid = positions <= length
        scores = jnp.einsum('grd,gsd->grs', q_row.astype(jnp.float32), keys.astype(jnp.float32)) * HEAD ** -0.5
        scores = jnp.where(valid, scores, -jnp.inf)
        weights = jnp.exp(scores - jnp.max(scores, axis=-1, keepdims=True))
        total = jnp.sum(weights, axis=-1, keepdims=True)
        mixed = jnp.einsum('grs,gsd->grd', weights.astype(jnp.bfloat16).astype(jnp.float32), values.astype(jnp.float32))
        return (mixed / total).astype(jnp.bfloat16)

    attended = lax.map(attend, (query, k_out, v_out, seq_lens)).reshape(BATCH, HEADS * HEAD)
    mid_hidden = (hidden.astype(jnp.float32) + jnp.dot(attended, w_o, preferred_element_type=jnp.float32)).astype(jnp.bfloat16)
    normed_mid = rms_norm(mid_hidden, mlp_norm)
    gate_proj = jnp.dot(normed_mid, w_gate, preferred_element_type=jnp.float32)
    up_proj = jnp.dot(normed_mid, w_up, preferred_element_type=jnp.float32)
    activated = (jax.nn.silu(gate_proj) * up_proj).astype(jnp.bfloat16)
    hidden_out = (mid_hidden.astype(jnp.float32) + jnp.dot(activated, w_down, preferred_element_type=jnp.float32)).astype(jnp.bfloat16)
    return (hidden_out, k_out, v_out)
```

```python
import functools
import jax
import jax.numpy as jnp
from jax import lax
from jax.experimental import pallas as pl
from jax.experimental.pallas import tpu as pltpu
from jax.sharding import PartitionSpec as P

NORM_EPS = 1e-6
MASK_VALUE = -3e38
F32 = jnp.float32
BF16 = jnp.bfloat16
MESH = pl.DeviceIdType.MESH
CORES = 2
COLS = 256
VMEM_LIMIT = 66_000_000


def dot32(a, b):
    return jnp.dot(a, b, preferred_element_type=F32)


def attn_kernel(lens, hid, gain, wq, wk, wv, kc, vc, o_out, st_out, k_out, v_out,
                hbuf, gbuf, ubuf, wbuf, qbuf, knew, vnew, kbuf, vbuf, obuf,
                hsem, wsem, kin, vin, kos, vos):
    rows, groups, blk, dim = kc.shape
    heads = wq.shape[1] // dim
    rep = heads // groups
    nq = wq.shape[1] // COLS
    nkv = wk.shape[1] // COLS
    nchunk = kin.shape[0]
    crow = rows // nchunk
    base = lax.axis_index('sp') * blk

    def load(i):
        r = pl.ds(i * crow, crow)
        return (pltpu.make_async_copy(kc.at[r], kbuf.at[r], kin.at[i]),
                pltpu.make_async_copy(vc.at[r], vbuf.at[r], vin.at[i]))

    def store(i):
        r = pl.ds(i * crow, crow)
        return (pltpu.make_async_copy(kbuf.at[r], k_out.at[r], kos.at[i]),
                pltpu.make_async_copy(vbuf.at[r], v_out.at[r], vos.at[i]))

    hcopy = pltpu.make_async_copy(hid, hbuf, hsem.at[0])
    gcopy = pltpu.make_async_copy(gain, gbuf, hsem.at[1])
    hcopy.start()
    gcopy.start()
    wcopies = []
    for src, n in ((wq, nq), (wk, nkv), (wv, nkv)):
        for j in range(n):
            t = len(wcopies)
            wcopies.append(pltpu.make_async_copy(src.at[:, pl.ds(j * COLS, COLS)], wbuf.at[t], wsem.at[t]))
    for cp in wcopies:
        cp.start()
    for i in range(2):
        for cp in load(i):
            cp.start()
    hcopy.wait()
    gcopy.wait()
    g = gbuf[...].astype(F32)
    for r in range(0, rows, 16):
        wide = hbuf[r:r + 16, :].astype(F32)
        inv = lax.rsqrt(jnp.mean(wide * wide, axis=-1, keepdims=True) + NORM_EPS)
        ubuf[r:r + 16, :] = (wide * inv * g).astype(BF16)

    issued = 2
    for t, cp in enumerate(wcopies):
        cp.wait()
        if issued < nchunk:
            for c2 in load(issued):
                c2.start()
            issued += 1
        res = dot32(ubuf[...], wbuf[t])
        per = COLS // dim
        for s in range(per):
            part = res[:, s * dim:(s + 1) * dim]
            if t < nq:
                qbuf[pl.ds(t * per + s, rows, stride=heads), :] = part
            elif t < nq + nkv:
                knew[(t - nq) * per + s] = part
            else:
                vnew[(t - nq - nkv) * per + s] = part
    while issued < nchunk:
        for c2 in load(issued):
            c2.start()
        issued += 1

    pair = 2 * heads
    row_id = lax.broadcasted_iota(jnp.int32, (pair, blk), 0)
    lane_id = lax.broadcasted_iota(jnp.int32, (pair, blk), 1)
    first = row_id < heads
    low = (row_id % heads) < rep
    stat_lane = lax.broadcasted_iota(jnp.int32, (heads, rows), 1)
    tile_row = lax.broadcasted_iota(jnp.int32, (16, dim), 0)
    scale = dim ** -0.5

    def chunk(i, carry):
        m_acc, l_acc = carry
        for cp in load(i):
            cp.wait()

        def patch(r, _):
            b = i * crow + r
            off = lens[b] - base
            hit = jnp.logical_and(off >= 0, off < blk)
            offc = jnp.clip(off, 0, blk - 1)
            t16 = pl.multiple_of((offc // 16) * 16, 16)
            want = jnp.where(hit, offc - t16, -1)
            mask = tile_row == want
            for gi in range(groups):
                kt = kbuf[b, gi, pl.ds(t16, 16), :]
                kbuf[b, gi, pl.ds(t16, 16), :] = jnp.where(mask, jnp.broadcast_to(knew[gi, pl.ds(b, 1), :], (16, dim)).astype(BF16), kt)
                vt = vbuf[b, gi, pl.ds(t16, 16), :]
                vbuf[b, gi, pl.ds(t16, 16), :] = jnp.where(mask, jnp.broadcast_to(vnew[gi, pl.ds(b, 1), :], (16, dim)).astype(BF16), vt)
            return 0

        lax.fori_loop(0, crow, patch, 0)
        for cp in store(i):
            cp.start()

        for r in range(0, crow, 2):
            b = i * crow + r
            q16 = qbuf[pl.ds(pl.multiple_of(b * heads, pair), pair), :]
            lhs = jnp.concatenate([jnp.where(first, q16, 0.0), jnp.where(first, 0.0, q16)], axis=1).astype(BF16)
            keys = jnp.concatenate([kbuf[b].reshape(groups * blk, dim), kbuf[b + 1].reshape(groups * blk, dim)], axis=1)
            sc = lax.dot_general(lhs, keys, (((1,), (1,)), ((), ())), preferred_element_type=F32)
            s = jnp.where(low, sc[:, :blk], sc[:, blk:]) * scale
            limit = jnp.where(first, lens[b] - base, lens[b + 1] - base)
            valid = lane_id <= limit
            s = jnp.where(valid, s, MASK_VALUE)
            m = jnp.max(s, axis=1, keepdims=True)
            p = jnp.where(valid, jnp.exp(s - m), 0.0)
            tot = jnp.sum(p, axis=1, keepdims=True)
            pcat = jnp.concatenate([jnp.where(low, p, 0.0), jnp.where(low, 0.0, p)], axis=1).astype(BF16)
            vals = jnp.concatenate([vbuf[b].reshape(groups * blk, dim), vbuf[b + 1].reshape(groups * blk, dim)], axis=1)
            mix = dot32(pcat, vals)
            obuf[pl.ds(pl.multiple_of(b * heads, pair), heads), :] = mix[:heads, :dim]
            obuf[pl.ds(pl.multiple_of(b * heads + heads, heads), heads), :] = mix[heads:, dim:]
            m_acc = jnp.where(stat_lane == b, m[:heads], jnp.where(stat_lane == b + 1, m[heads:], m_acc))
            l_acc = jnp.where(stat_lane == b, tot[:heads], jnp.where(stat_lane == b + 1, tot[heads:], l_acc))
        return m_acc, l_acc

    zero = jnp.zeros((heads, rows), F32)
    m_acc, l_acc = lax.fori_loop(0, nchunk, chunk, (zero, zero))
    half = heads // CORES
    for ci in range(CORES):
        st_out[ci] = jnp.concatenate([m_acc[ci * half:(ci + 1) * half], l_acc[ci * half:(ci + 1) * half]], axis=0)
    for h in range(heads):
        o_out[h] = obuf[pl.ds(h, rows, stride=heads), :]

    def drain(i, _):
        for cp in store(i):
            cp.wait()
        return 0

    lax.fori_loop(0, nchunk, drain, 0)


def attention(hidden, seq_lens, k_cache, v_cache, gain, w_q, w_k, w_v):
    rows, groups, blk, dim = k_cache.shape
    heads = w_q.shape[1] // dim
    width = w_q.shape[0]
    nw = (w_q.shape[1] + w_k.shape[1] + w_v.shape[1]) // COLS
    nchunk = 8
    any_spec = pl.BlockSpec(memory_space=pl.ANY)
    vm = pl.BlockSpec(memory_space=pltpu.VMEM)
    return pl.pallas_call(
        attn_kernel,
        name='block_attention',
        out_shape=(jax.ShapeDtypeStruct((heads, rows, dim), F32),
                   jax.ShapeDtypeStruct((CORES, heads, rows), F32),
                   jax.ShapeDtypeStruct(k_cache.shape, BF16),
                   jax.ShapeDtypeStruct(v_cache.shape, BF16)),
        in_specs=[pl.BlockSpec(memory_space=pltpu.SMEM)] + [any_spec] * 7,
        out_specs=(vm, vm, any_spec, any_spec),
        scratch_shapes=[
            pltpu.VMEM((rows, width), BF16),
            pltpu.VMEM((1, width), BF16),
            pltpu.VMEM((rows, width), BF16),
            pltpu.VMEM((nw, width, COLS), BF16),
            pltpu.VMEM((rows * heads, dim), F32),
            pltpu.VMEM((groups, rows, dim), F32),
            pltpu.VMEM((groups, rows, dim), F32),
            pltpu.VMEM(k_cache.shape, BF16),
            pltpu.VMEM(v_cache.shape, BF16),
            pltpu.VMEM((rows * heads, dim), F32),
            pltpu.SemaphoreType.DMA((2,)),
            pltpu.SemaphoreType.DMA((nw,)),
            pltpu.SemaphoreType.DMA((nchunk,)),
            pltpu.SemaphoreType.DMA((nchunk,)),
            pltpu.SemaphoreType.DMA((nchunk,)),
            pltpu.SemaphoreType.DMA((nchunk,)),
        ],
        compiler_params=pltpu.CompilerParams(vmem_limit_bytes=VMEM_LIMIT),
    )(seq_lens, hidden, gain.reshape(1, width), w_q, w_k, w_v, k_cache, v_cache)


def mlp_kernel(nx, ny, hid, o_in, st_in, gain, wo, wg, wu, wd, out,
               wo_b, wg_b, wu_b, wd_b, hid_b, gain_b, o_b, st_b, po_b, pst_b, oc_b, cst_b, xo_b, xst_b, tst_b,
               att_b, pw_b, rw_b, mid_b, u2_b, act_b, ab_b, pd_b, rd_b, fin_b,
               lsem, wsem, ds_s, ds_r, xs_s, xs_r, as_s, as_r, ws_s, ws_r, ms_s, ms_r, cs_s, cs_r, dn_s, dn_r, fs_s, fs_r, fp_s, fp_r):
    sp = lax.axis_index('sp')
    y = lax.axis_index('tp')
    x = sp // CORES
    c = sp % CORES
    oc = 1 - c
    half_h, rows, dim = po_b.shape
    xr = rows // nx
    width = gain.shape[1]
    hw = width // CORES
    cw = hw // ny
    partner = {'tp': y, 'sp': x * CORES + oc}

    def peer(yy, xx):
        return {'tp': yy, 'sp': xx * CORES + c}

    def rcopy(src, dst, ssem, rsem, dev):
        return pltpu.make_async_remote_copy(src_ref=src, dst_ref=dst, send_sem=ssem, recv_sem=rsem, device_id=dev, device_id_type=MESH)

    def cols(i, n):
        return pl.ds(pl.multiple_of(i * n, n), n)

    loads = [
        pltpu.make_async_copy(o_in, o_b, lsem.at[0]),
        pltpu.make_async_copy(st_in, st_b, lsem.at[1]),
        pltpu.make_async_copy(hid.at[pl.ds(x * xr, xr), pl.ds(pl.multiple_of(c * hw + y * cw, cw), cw)], hid_b, lsem.at[2]),
        pltpu.make_async_copy(gain, gain_b, lsem.at[3]),
    ]
    for cp in loads:
        cp.start()
    inner = wg_b.shape[1]
    w_loads = [
        pltpu.make_async_copy(wo.at[:, cols(c, hw)], wo_b, wsem.at[0]),
        pltpu.make_async_copy(wg.at[:, cols(c, inner)], wg_b, wsem.at[1]),
        pltpu.make_async_copy(wu.at[:, cols(c, inner)], wu_b, wsem.at[2]),
        pltpu.make_async_copy(wd.at[:, cols(c, hw)], wd_b, wsem.at[3]),
    ]
    for cp in w_loads:
        cp.start()

    barrier = pltpu.get_barrier_semaphore()
    pl.semaphore_signal(barrier, inc=1, device_id=partner, device_id_type=MESH)
    for k in range(1, nx):
        pl.semaphore_signal(barrier, inc=1, device_id=peer(y, (x + k) % nx), device_id_type=MESH)
    for k in range(1, ny):
        pl.semaphore_signal(barrier, inc=1, device_id=peer((y + k) % ny, x), device_id_type=MESH)
    for cp in loads:
        cp.wait()
    pl.semaphore_wait(barrier, 1 + (nx - 1) + (ny - 1))

    d2d = [rcopy(o_b.at[pl.ds(half_h * oc, half_h)], po_b, ds_s.at[0], ds_r.at[0], partner),
           rcopy(st_b.at[oc], pst_b, ds_s.at[1], ds_r.at[1], partner)]
    for cp in d2d:
        cp.start()
    for cp in d2d:
        cp.wait()
    s0 = st_b[c]
    s1 = pst_b[...]
    m0, l0, m1, l1 = s0[:half_h], s0[half_h:], s1[:half_h], s1[half_h:]
    mm = jnp.maximum(m0, m1)
    a0, a1 = jnp.exp(m0 - mm), jnp.exp(m1 - mm)
    cst_b[...] = jnp.concatenate([mm, a0 * l0 + a1 * l1], axis=0)
    tr = jnp.concatenate([a0, a1], axis=0).T
    for h in range(half_h):
        oc_b[h] = o_b[half_h * c + h] * tr[:, h:h + 1] + po_b[h] * tr[:, half_h + h:half_h + h + 1]

    sends = []
    for k in range(1, nx):
        xx = (x + k) % nx
        sends.append(rcopy(cst_b, xst_b.at[x], xs_s.at[k - 1, 0], xs_r.at[x, 0], peer(y, xx)))
        sends.append(rcopy(oc_b.at[:, pl.ds(xx * xr, xr), :], xo_b.at[x], xs_s.at[k - 1, 1], xs_r.at[x, 1], peer(y, xx)))
    for cp in sends:
        cp.start()
    tst_b[0] = cst_b[...].T
    for k in range(1, nx):
        xx = (x + k) % nx
        rcopy(cst_b, xst_b.at[xx], xs_s.at[k - 1, 0], xs_r.at[xx, 0], peer(y, xx)).wait_recv()
        tst_b[k] = xst_b[xx].T
    stats = [tst_b[k, pl.ds(x * xr, xr), :] for k in range(nx)]
    mm = stats[0][:, :half_h]
    for k in range(1, nx):
        mm = jnp.maximum(mm, stats[k][:, :half_h])
    alphas = [jnp.exp(st[:, :half_h] - mm) for st in stats]
    total = alphas[0] * stats[0][:, half_h:]
    for k in range(1, nx):
        total = total + alphas[k] * stats[k][:, half_h:]
    for k in range(1, nx):
        xx = (x + k) % nx
        rcopy(oc_b.at[:, pl.ds(xx * xr, xr), :], xo_b.at[xx], xs_s.at[k - 1, 1], xs_r.at[xx, 1], peer(y, xx)).wait_recv()
    for h in range(half_h):
        acc = oc_b[h, pl.ds(x * xr, xr), :] * alphas[0][:, h:h + 1]
        for k in range(1, nx):
            acc = acc + xo_b[(x + k) % nx, h] * alphas[k][:, h:h + 1]
        att_b[c, :, h * dim:(h + 1) * dim] = (acc / total[:, h:h + 1]).astype(BF16).astype(F32)
    swap = rcopy(att_b.at[c], att_b.at[c], as_s.at[0], as_r.at[0], partner)
    swap.start()
    for cp in sends:
        cp.wait_send()
    rcopy(att_b.at[oc], att_b.at[oc], as_s.at[0], as_r.at[0], partner).wait_recv()
    swap.wait_send()

    def reduce_y(lhs_of, w_b, send_b, recv_b, s_sem, r_sem):
        lhs = lhs_of()
        started = []
        for k in [2, 1, 3, 0] if ny == 4 else list(range(1, ny)) + [0]:
            yy = (y + k) % ny
            send_b[yy] = dot32(lhs, w_b[:, cols(yy, cw)])
            if k:
                cp = rcopy(send_b.at[yy], recv_b.at[y], s_sem.at[k], r_sem.at[y], peer(yy, x))
                cp.start()
                started.append(cp)
        total = send_b[y]
        for k in range(1, ny):
            yy = (y + k) % ny
            rcopy(send_b.at[yy], recv_b.at[yy], s_sem.at[k], r_sem.at[yy], peer(yy, x)).wait_recv()
            total = total + recv_b[yy]
        for cp in started:
            cp.wait_send()
        return total

    w_loads[0].wait()
    total = reduce_y(lambda: jnp.concatenate([att_b[0], att_b[1]], axis=1).astype(BF16), wo_b, pw_b, rw_b, ws_s, ws_r)
    mid_b[c, y] = (hid_b[...].astype(F32) + total).astype(BF16).astype(F32)

    started = [rcopy(mid_b.at[c, y], mid_b.at[c, y], cs_s.at[0], cs_r.at[y], partner)]
    for k in range(1, ny):
        yy = (y + k) % ny
        started.append(rcopy(mid_b.at[c, y], mid_b.at[c, y], ms_s.at[k], ms_r.at[y], peer(yy, x)))
    for cp in started:
        cp.start()
    for k in range(1, ny):
        yy = (y + k) % ny
        rcopy(mid_b.at[c, yy], mid_b.at[c, yy], ms_s.at[k], ms_r.at[yy], peer(yy, x)).wait_recv()
        cp = rcopy(mid_b.at[c, yy], mid_b.at[c, yy], cs_s.at[k], cs_r.at[yy], partner)
        cp.start()
        started.append(cp)
    for k in range(ny):
        yy = (y + k) % ny
        rcopy(mid_b.at[oc, yy], mid_b.at[oc, yy], cs_s.at[k], cs_r.at[yy], partner).wait_recv()
    sq = jnp.zeros((xr, 1), F32)
    for ci in range(CORES):
        for yi in range(ny):
            v = mid_b[ci, yi]
            sq = sq + jnp.sum(v * v, axis=-1, keepdims=True)
    inv = lax.rsqrt(sq / width + NORM_EPS)
    for ci in range(CORES):
        for yi in range(ny):
            o = ci * hw + yi * cw
            u2_b[:, o:o + cw] = (mid_b[ci, yi] * inv * gain_b[:, o:o + cw].astype(F32)).astype(BF16)
    for cp in started:
        cp.wait_send()

    w_loads[1].wait()
    w_loads[2].wait()
    steps = inner // COLS

    def gate_up(j, _):
        lhs = u2_b[...]
        gp = dot32(lhs, wg_b[:, cols(j, COLS)])
        up = dot32(lhs, wu_b[:, cols(j, COLS)])
        act_b[c, j] = (gp * jax.nn.sigmoid(gp) * up).astype(BF16).astype(F32)
        rcopy(act_b.at[c, j], act_b.at[c, j], dn_s.at[j], dn_r.at[j], partner).start()
        return 0

    lax.fori_loop(0, steps, gate_up, 0)

    def take(j, _):
        rcopy(act_b.at[oc, j], act_b.at[oc, j], dn_s.at[j], dn_r.at[j], partner).wait()
        for ci in range(CORES):
            ab_b[:, pl.ds(pl.multiple_of(ci * inner + j * COLS, COLS), COLS)] = act_b[ci, j].astype(BF16)
        return 0

    lax.fori_loop(0, steps, take, 0)
    w_loads[3].wait()
    total = reduce_y(lambda: ab_b[...], wd_b, pd_b, rd_b, fs_s, fs_r)
    fin_b[x, y, c] = (mid_b[c, y] + total).astype(BF16).astype(F32)

    def slot(yy, xx):
        return fin_b.at[xx, yy, c]

    def place(k1, k2):
        return (y + k1 * oc + k2 * c) % ny, (x + k1 * c + k2 * oc) % nx

    started = []

    def spread(k1):
        sy, sx = place(k1, 0)
        for k2 in [2, 1, 3] if nx == 4 else range(1, nx):
            ty, tx = place(0, k2)
            cp = rcopy(slot(sy, sx), slot(sy, sx), fp_s.at[k1, k2], fp_r.at[sx, sy, c], peer(ty, tx))
            cp.start()
            started.append(cp)
        cp = rcopy(slot(sy, sx), slot(sy, sx), fp_s.at[k1, 0], fp_r.at[sx, sy, c], partner)
        cp.start()
        started.append(cp)

    for k1 in [2, 1, 3] if ny == 4 else range(1, ny):
        ty, tx = place(k1, 0)
        cp = rcopy(slot(y, x), slot(y, x), fp_s.at[0, nx + k1], fp_r.at[x, y, c], peer(ty, tx))
        cp.start()
        started.append(cp)
    spread(0)

    def arrived(yy, xx, ci):
        return rcopy(fin_b.at[xx, yy, ci], fin_b.at[xx, yy, ci], fp_s.at[0, 0], fp_r.at[xx, yy, ci], partner)

    for k1 in [1, 3, 2] if ny == 4 else range(1, ny):
        sy, sx = place(k1, 0)
        arrived(sy, sx, c).wait_recv()
        spread(k1)
    for k1 in [0, 1, 3, 2] if ny == 4 else range(ny):
        for k2 in [1, 3, 2] if nx == 4 else range(1, nx):
            sy, sx = place(k1, k2)
            arrived(sy, sx, c).wait_recv()
            cp = rcopy(slot(sy, sx), slot(sy, sx), fp_s.at[k1, nx + ny + k2], fp_r.at[sx, sy, c], partner)
            cp.start()
            started.append(cp)
    for xi in range(nx):
        for yi in range(ny):
            arrived(yi, xi, oc).wait_recv()
    for xi in range(nx):
        for yi in range(ny):
            for ci in range(CORES):
                o = ci * hw + yi * cw
                out[xi * xr:(xi + 1) * xr, o:o + cw] = fin_b[xi, yi, ci].astype(BF16)
    for cp in started:
        cp.wait_send()


def mlp(mesh, hidden, o_part, stats, gain, w_o, w_gate, w_up, w_down):
    rows, width = hidden.shape
    heads, _, dim = o_part.shape
    half_h = heads // CORES
    nx = mesh.shape['sp'] // CORES
    ny = mesh.shape['tp']
    xr = rows // nx
    hw = width // CORES
    cw = hw // ny
    inner = w_gate.shape[1] // CORES
    steps = inner // COLS
    any_spec = pl.BlockSpec(memory_space=pl.ANY)
    dma = pltpu.SemaphoreType.DMA
    return pl.pallas_call(
        functools.partial(mlp_kernel, nx, ny),
        name='exchange_mlp',
        out_shape=jax.ShapeDtypeStruct(hidden.shape, BF16),
        in_specs=[any_spec] * 8,
        out_specs=pl.BlockSpec(memory_space=pltpu.VMEM),
        scratch_shapes=[
            pltpu.VMEM((w_o.shape[0], hw), BF16),
            pltpu.VMEM((width, inner), BF16),
            pltpu.VMEM((width, inner), BF16),
            pltpu.VMEM((w_down.shape[0], hw), BF16),
            pltpu.VMEM((xr, cw), BF16),
            pltpu.VMEM((1, width), BF16),
            pltpu.VMEM((heads, rows, dim), F32),
            pltpu.VMEM((CORES, heads, rows), F32),
            pltpu.VMEM((half_h, rows, dim), F32),
            pltpu.VMEM((heads, rows), F32),
            pltpu.VMEM((half_h, rows, dim), F32),
            pltpu.VMEM((heads, rows), F32),
            pltpu.VMEM((nx, half_h, xr, dim), F32),
            pltpu.VMEM((nx, heads, rows), F32),
            pltpu.VMEM((nx, rows, heads), F32),
            pltpu.VMEM((CORES, xr, half_h * dim), F32),
            pltpu.VMEM((ny, xr, cw), F32),
            pltpu.VMEM((ny, xr, cw), F32),
            pltpu.VMEM((CORES, ny, xr, cw), F32),
            pltpu.VMEM((xr, width), BF16),
            pltpu.VMEM((CORES, steps, xr, COLS), F32),
            pltpu.VMEM((xr, CORES * inner), BF16),
            pltpu.VMEM((ny, xr, cw), F32),
            pltpu.VMEM((ny, xr, cw), F32),
            pltpu.VMEM((nx, ny, CORES, xr, cw), F32),
            dma((4,)), dma((4,)),
            dma((2,)), dma((2,)),
            dma((nx, 2)), dma((nx, 2)),
            dma((1,)), dma((1,)),
            dma((ny,)), dma((ny,)),
            dma((ny,)), dma((ny,)),
            dma((ny,)), dma((ny,)),
            dma((steps,)), dma((steps,)),
            dma((ny,)), dma((ny,)),
            dma((ny, 2 * nx + ny)), dma((nx, ny, CORES)),
        ],
        compiler_params=pltpu.CompilerParams(vmem_limit_bytes=VMEM_LIMIT, collective_id=0, has_side_effects=True),
    )(hidden, o_part, stats, gain.reshape(1, width), w_o, w_gate, w_up, w_down)


def solution(mesh):
    cache_spec = P('dp', 'tp', 'sp', None)
    row_spec = P('dp', None)
    col_spec = P(None, 'tp')
    inner_spec = P('tp', None)
    gain_spec = P(None)

    def local_step(hidden, seq_lens, k_cache, v_cache, attn_norm, w_q, w_k, w_v, w_o, mlp_norm, w_gate, w_up, w_down):
        o_part, stats, k_out, v_out = attention(hidden, seq_lens, k_cache, v_cache, attn_norm, w_q, w_k, w_v)
        hidden_out = mlp(mesh, hidden, o_part, stats, mlp_norm, w_o, w_gate, w_up, w_down)
        return hidden_out, k_out, v_out

    return jax.shard_map(local_step, mesh=mesh, in_specs=(row_spec, P('dp'), cache_spec, cache_spec, gain_spec, col_spec, col_spec, col_spec, inner_spec, gain_spec, col_spec, col_spec, inner_spec), out_specs=(row_spec, cache_spec, cache_spec), check_vma=False)
```

```python
import functools
import jax
import jax.numpy as jnp
from jax import lax
from jax.experimental import pallas as pl
from jax.experimental.pallas import tpu as pltpu
from jax.sharding import PartitionSpec as P

NORM_EPS = 1e-6
MASK_VALUE = -3e38
F32 = jnp.float32
BF16 = jnp.bfloat16
MESH = pl.DeviceIdType.MESH
CORES = 2
COLS = 256
LANES = 128
VMEM_LIMIT = 66_000_000


def dot32(a, b):
    return jnp.dot(a, b, preferred_element_type=F32)


def attn_kernel(lens_in, hid, gain, wq, wk, wv, kc, vc, o_out, st_out, k_out, v_out,
                lens, obuf, hbuf, gbuf, ubuf, wbuf, qbuf, knew, vnew, kbuf, vbuf, pbuf,
                hsem, wsem, kin, vin, kos, vos):
    rows, groups, blk, dim = kc.shape
    heads = wq.shape[1] // dim
    rep = heads // groups
    nq = wq.shape[1] // COLS
    nkv = wk.shape[1] // COLS
    nchunk = kin.shape[0]
    crow = rows // nchunk
    base = lax.axis_index('sp') * blk

    def load(i):
        r = pl.ds(i * crow, crow)
        return (pltpu.make_async_copy(kc.at[r], kbuf.at[r], kin.at[i]),
                pltpu.make_async_copy(vc.at[r], vbuf.at[r], vin.at[i]))

    def store(i):
        r = pl.ds(i * crow, crow)
        return (pltpu.make_async_copy(kbuf.at[r], k_out.at[r], kos.at[i]),
                pltpu.make_async_copy(vbuf.at[r], v_out.at[r], vos.at[i]))

    hcopy = pltpu.make_async_copy(hid, hbuf, hsem.at[0])
    gcopy = pltpu.make_async_copy(gain, gbuf, hsem.at[1])
    lcopy = pltpu.make_async_copy(lens_in, lens, hsem.at[2])
    lcopy.start()
    hcopy.start()
    gcopy.start()
    per = COLS // dim

    def weight(src, j, t):
        return pltpu.make_async_copy(src.at[:, pl.ds(j * COLS, COLS)], wbuf.at[t], wsem.at[t])

    weights = [weight(wk, j, j) for j in range(nkv)] + [weight(wv, j, nkv + j) for j in range(nkv)]
    weights += [weight(wq, j, 2 * nkv + j) for j in range(nq)]
    for cp in weights:
        cp.start()
    issued = 1
    for i in range(issued):
        for cp in load(i):
            cp.start()
    lcopy.wait()
    hcopy.wait()
    gcopy.wait()
    g_rows = gbuf[...].astype(F32)
    for r in range(0, rows, 16):
        wide = hbuf[r:r + 16, :].astype(F32)
        inv = lax.rsqrt(jnp.mean(wide * wide, axis=-1, keepdims=True) + NORM_EPS)
        for j in range(gbuf.shape[0]):
            sl = slice(j * LANES, (j + 1) * LANES)
            ubuf[r:r + 16, sl] = (wide[:, sl] * inv * g_rows[j:j + 1, :]).astype(BF16)

    for t, cp in enumerate(weights):
        cp.wait()
        if issued < nchunk:
            for c2 in load(issued):
                c2.start()
            issued += 1
        res = dot32(ubuf[...], wbuf[t])
        for s in range(per):
            part = res[:, s * dim:(s + 1) * dim]
            if t < nkv:
                knew[t * per + s] = part
            elif t < 2 * nkv:
                vnew[(t - nkv) * per + s] = part
            else:
                qbuf[(t - 2 * nkv) * per + s] = part

    tile_row = lax.broadcasted_iota(jnp.int32, (16, dim), 0)

    def update(i):
        for cp in load(i):
            cp.wait()

        def patch(r, _):
            b = i * crow + r
            off = lens[b] - base
            hit = jnp.logical_and(off >= 0, off < blk)
            offc = jnp.clip(off, 0, blk - 1)
            t16 = pl.multiple_of((offc // 16) * 16, 16)
            want = jnp.where(hit, offc - t16, -1)
            mask = tile_row == want
            for gi in range(groups):
                kt = kbuf[b, gi, pl.ds(t16, 16), :]
                kbuf[b, gi, pl.ds(t16, 16), :] = jnp.where(mask, jnp.broadcast_to(knew[gi, pl.ds(b, 1), :], (16, dim)).astype(BF16), kt)
                vt = vbuf[b, gi, pl.ds(t16, 16), :]
                vbuf[b, gi, pl.ds(t16, 16), :] = jnp.where(mask, jnp.broadcast_to(vnew[gi, pl.ds(b, 1), :], (16, dim)).astype(BF16), vt)
            return 0

        lax.fori_loop(0, crow, patch, 0, unroll=4)
        for cp in store(i):
            cp.start()

    ahead = 2
    for i in range(ahead):
        update(i)

    slot_id = lax.broadcasted_iota(jnp.int32, (blk, rep * crow), 0)
    lane_b = lax.broadcasted_iota(jnp.int32, (1, heads * crow), 1) % crow
    low = lax.broadcasted_iota(jnp.int32, (heads, blk), 0) < rep
    scale = dim ** -0.5
    ms, ls = [], []

    for i in range(nchunk):
        if i + ahead < nchunk:
            update(i + ahead)
        b0 = i * crow
        qt = jnp.concatenate([qbuf[h, b0:b0 + crow, :] for h in range(heads)], axis=0).T
        limit = jnp.zeros((1, heads * crow), jnp.int32)
        for r in range(crow):
            limit = jnp.where(lane_b == r, lens[b0 + r] - base, limit)
        rhs = [jnp.concatenate([jnp.where(lane_b[:, :rep * crow] == r, qt[:, gi * rep * crow:(gi + 1) * rep * crow], 0.0).astype(BF16) for r in range(crow)], axis=0) for gi in range(groups)]
        sts = [dot32(jnp.concatenate([kbuf[b0 + r, gi] for r in range(crow)], axis=1), rhs[gi]) for gi in range(groups)]
        mrow, lrow = [], []
        for gi in range(groups):
            lanes = slice(gi * rep * crow, (gi + 1) * rep * crow)
            s = sts[gi] * scale
            valid = slot_id <= limit[:, lanes]
            s = jnp.where(valid, s, MASK_VALUE)
            m = jnp.max(s, axis=0, keepdims=True)
            p = jnp.where(valid, jnp.exp(s - m), 0.0)
            mrow.append(m)
            lrow.append(jnp.sum(p, axis=0, keepdims=True))
            pbuf[gi * rep * crow:(gi + 1) * rep * crow, :] = p.T
        ms.append(mrow)
        ls.append(lrow)
        for r in range(0, crow, 2):
            lhs = []
            for q in range(2):
                ps = pbuf[pl.ds(r + q, heads, stride=crow), :]
                lhs.append(jnp.concatenate([jnp.where(low, ps, 0.0), jnp.where(low, 0.0, ps)], axis=1))
            vals = jnp.concatenate([vbuf[b0 + r].reshape(groups * blk, dim), vbuf[b0 + r + 1].reshape(groups * blk, dim)], axis=1)
            mix = dot32(jnp.concatenate(lhs, axis=0).astype(BF16), vals)
            obuf[pl.ds(b0 + r, heads, stride=rows), :] = mix[:heads, :dim]
            obuf[pl.ds(b0 + r + 1, heads, stride=rows), :] = mix[heads:, dim:]

    ocopy = pltpu.make_async_copy(obuf, o_out, hsem.at[3])
    ocopy.start()
    half = heads // CORES
    for ci in range(CORES):
        for h in range(half):
            gi, ri = divmod(ci * half + h, rep)
            lanes = slice(ri * crow, (ri + 1) * crow)
            st_out[ci, h:h + 1, :] = jnp.concatenate([mrow[gi][:, lanes] for mrow in ms], axis=1)
            st_out[ci, half + h:half + h + 1, :] = jnp.concatenate([lrow[gi][:, lanes] for lrow in ls], axis=1)

    def drain(i, _):
        for cp in store(i):
            cp.wait()
        return 0

    ocopy.wait()
    lax.fori_loop(0, nchunk, drain, 0)


def attention(hidden, seq_lens, k_cache, v_cache, gain, w_q, w_k, w_v):
    rows, groups, blk, dim = k_cache.shape
    heads = w_q.shape[1] // dim
    width = w_q.shape[0]
    nw = (w_q.shape[1] + w_k.shape[1] + w_v.shape[1]) // COLS
    nchunk = 4
    any_spec = pl.BlockSpec(memory_space=pl.ANY)
    vm = pl.BlockSpec(memory_space=pltpu.VMEM)
    return pl.pallas_call(
        attn_kernel,
        name='block_attention',
        out_shape=(jax.ShapeDtypeStruct((heads * rows, dim), F32),
                   jax.ShapeDtypeStruct((CORES, heads, rows), F32),
                   jax.ShapeDtypeStruct(k_cache.shape, BF16),
                   jax.ShapeDtypeStruct(v_cache.shape, BF16)),
        in_specs=[any_spec] * 8,
        out_specs=(any_spec, vm, any_spec, any_spec),
        scratch_shapes=[
            pltpu.SMEM((rows,), jnp.int32),
            pltpu.VMEM((heads * rows, dim), F32),
            pltpu.VMEM((rows, width), BF16),
            pltpu.VMEM((width // LANES, LANES), BF16),
            pltpu.VMEM((rows, width), BF16),
            pltpu.VMEM((nw, width, COLS), BF16),
            pltpu.VMEM((heads, rows, dim), F32),
            pltpu.VMEM((groups, rows, dim), F32),
            pltpu.VMEM((groups, rows, dim), F32),
            pltpu.VMEM(k_cache.shape, BF16),
            pltpu.VMEM(v_cache.shape, BF16),
            pltpu.VMEM((heads * rows // nchunk, blk), F32),
            pltpu.SemaphoreType.DMA((4,)),
            pltpu.SemaphoreType.DMA((nw,)),
            pltpu.SemaphoreType.DMA((nchunk,)),
            pltpu.SemaphoreType.DMA((nchunk,)),
            pltpu.SemaphoreType.DMA((nchunk,)),
            pltpu.SemaphoreType.DMA((nchunk,)),
        ],
        compiler_params=pltpu.CompilerParams(vmem_limit_bytes=VMEM_LIMIT),
    )(seq_lens, hidden, gain.reshape(width // LANES, LANES), w_q, w_k, w_v, k_cache, v_cache)


def mlp_kernel(nx, ny, hid, o_in, st_in, gain, wo, wg, wu, wd, out,
               wo_b, wg_b, wu_b, wd_b, hid_b, gain_b, o_b, st_b, po_b, pst_b, oc_b, cst_b, xo_b, xst_b, tst_b,
               att_b, pw_b, rw_b, mid_b, u2_b, act_b, ab_b, pd_b, rd_b, fin_b,
               lsem, osem, gsem, usem, dsem, ds_s, ds_r, xs_s, xs_r, as_s, as_r, ws_s, ws_r, ms_s, ms_r, cs_s, cs_r, dn_s, dn_r, fs_s, fs_r, fp_s, fp_r):
    sp = lax.axis_index('sp')
    y = lax.axis_index('tp')
    x = sp // CORES
    c = sp % CORES
    oc = 1 - c
    half_h, rows, dim = po_b.shape
    xr = rows // nx
    width = gain.shape[0] * LANES
    hw = width // CORES
    cw = hw // ny
    partner = {'tp': y, 'sp': x * CORES + oc}

    def peer(yy, xx):
        return {'tp': yy, 'sp': xx * CORES + c}

    def rcopy(src, dst, ssem, rsem, dev):
        return pltpu.make_async_remote_copy(src_ref=src, dst_ref=dst, send_sem=ssem, recv_sem=rsem, device_id=dev, device_id_type=MESH)

    def cols(i, n):
        return pl.ds(pl.multiple_of(i * n, n), n)

    loads = [
        pltpu.make_async_copy(o_in, o_b, lsem.at[0]),
        pltpu.make_async_copy(st_in, st_b, lsem.at[1]),
        pltpu.make_async_copy(hid.at[pl.ds(x * xr, xr), pl.ds(pl.multiple_of(c * hw + y * cw, cw), cw)], hid_b, lsem.at[2]),
        pltpu.make_async_copy(gain, gain_b, lsem.at[3]),
    ]
    for cp in loads:
        cp.start()
    steps = wg_b.shape[0]
    inner = steps * COLS
    def row_load(w, w_b, sem, n, j):
        r = cols(j, w_b.shape[0] // n)
        return pltpu.make_async_copy(w.at[r, cols(c, hw)], w_b.at[r], sem.at[j])

    def col_loads(j):
        r = cols(c * steps + j, COLS)
        return (pltpu.make_async_copy(wg.at[:, r], wg_b.at[j], gsem.at[j]), pltpu.make_async_copy(wu.at[:, r], wu_b.at[j], usem.at[j]))

    wo_loads = [row_load(wo, wo_b, osem, osem.shape[0], j) for j in range(osem.shape[0])]
    wd_loads = [row_load(wd, wd_b, dsem, steps, j) for j in range(steps)]
    for cp in wo_loads:
        cp.start(priority=1)
    for cp in col_loads(0):
        cp.start(priority=1)
    for cp in col_loads(1):
        cp.start(priority=1)
    for cp in col_loads(2):
        cp.start(priority=1)

    barrier = pltpu.get_barrier_semaphore()
    pl.semaphore_signal(barrier, inc=1, device_id=partner, device_id_type=MESH)
    for k in range(1, nx):
        pl.semaphore_signal(barrier, inc=1, device_id=peer(y, (x + k) % nx), device_id_type=MESH)
    for k in range(1, ny):
        pl.semaphore_signal(barrier, inc=1, device_id=peer((y + k) % ny, x), device_id_type=MESH)
    for cp in loads:
        cp.wait()
    pl.semaphore_wait(barrier, 1 + (nx - 1) + (ny - 1))

    d2d = [rcopy(o_b.at[pl.ds(half_h * oc, half_h)], po_b, ds_s.at[0], ds_r.at[0], partner),
           rcopy(st_b.at[oc], pst_b, ds_s.at[1], ds_r.at[1], partner)]
    for cp in d2d:
        cp.start()
    for cp in d2d:
        cp.wait()
    s0 = st_b[c]
    s1 = pst_b[...]
    m0, l0, m1, l1 = s0[:half_h], s0[half_h:], s1[:half_h], s1[half_h:]
    mm = jnp.maximum(m0, m1)
    a0, a1 = jnp.exp(m0 - mm), jnp.exp(m1 - mm)
    cst_b[...] = jnp.concatenate([mm, a0 * l0 + a1 * l1], axis=0)
    tr = jnp.concatenate([a0, a1], axis=0).T
    for h in range(half_h):
        oc_b[h] = o_b[half_h * c + h] * tr[:, h:h + 1] + po_b[h] * tr[:, half_h + h:half_h + h + 1]

    sends = []
    for k in range(1, nx):
        xx = (x + k) % nx
        sends.append(rcopy(cst_b, xst_b.at[x], xs_s.at[k - 1, 0], xs_r.at[x, 0], peer(y, xx)))
        sends.append(rcopy(oc_b.at[:, pl.ds(xx * xr, xr), :], xo_b.at[x], xs_s.at[k - 1, 1], xs_r.at[x, 1], peer(y, xx)))
    for cp in sends:
        cp.start()
    for cp in col_loads(3):
        cp.start(priority=1)
    for cp in col_loads(4):
        cp.start(priority=1)
    tst_b[0] = cst_b[...].T
    for k in range(1, nx):
        xx = (x + k) % nx
        rcopy(cst_b, xst_b.at[xx], xs_s.at[k - 1, 0], xs_r.at[xx, 0], peer(y, xx)).wait_recv()
        tst_b[k] = xst_b[xx].T
    stats = [tst_b[k, pl.ds(x * xr, xr), :] for k in range(nx)]
    mm = stats[0][:, :half_h]
    for k in range(1, nx):
        mm = jnp.maximum(mm, stats[k][:, :half_h])
    alphas = [jnp.exp(st[:, :half_h] - mm) for st in stats]
    total = alphas[0] * stats[0][:, half_h:]
    for k in range(1, nx):
        total = total + alphas[k] * stats[k][:, half_h:]
    for k in range(1, nx):
        xx = (x + k) % nx
        rcopy(oc_b.at[:, pl.ds(xx * xr, xr), :], xo_b.at[xx], xs_s.at[k - 1, 1], xs_r.at[xx, 1], peer(y, xx)).wait_recv()
    for h in range(half_h):
        acc = oc_b[h, pl.ds(x * xr, xr), :] * alphas[0][:, h:h + 1]
        for k in range(1, nx):
            acc = acc + xo_b[(x + k) % nx, h] * alphas[k][:, h:h + 1]
        att_b[c, :, h * dim:(h + 1) * dim] = (acc / total[:, h:h + 1]).astype(BF16).astype(F32)
    swap = rcopy(att_b.at[c], att_b.at[c], as_s.at[0], as_r.at[0], partner)
    swap.start()
    for cp in sends:
        cp.wait_send()
    rcopy(att_b.at[oc], att_b.at[oc], as_s.at[0], as_r.at[0], partner).wait_recv()
    swap.wait_send()

    def reduce_y(lhs_of, w_b, send_b, recv_b, s_sem, r_sem):
        lhs = lhs_of()
        started = []
        for k in [2, 1, 3, 0] if ny == 4 else list(range(1, ny)) + [0]:
            yy = (y + k) % ny
            send_b[yy] = dot32(lhs, w_b[:, cols(yy, cw)])
            if k:
                cp = rcopy(send_b.at[yy], recv_b.at[y], s_sem.at[k], r_sem.at[y], peer(yy, x))
                cp.start()
                started.append(cp)
        total = send_b[y]
        for k in range(1, ny):
            yy = (y + k) % ny
            rcopy(send_b.at[yy], recv_b.at[yy], s_sem.at[k], r_sem.at[yy], peer(yy, x)).wait_recv()
            total = total + recv_b[yy]
        for cp in started:
            cp.wait_send()
        return total

    for cp in wo_loads:
        cp.wait()
    total = reduce_y(lambda: jnp.concatenate([att_b[0], att_b[1]], axis=1).astype(BF16), wo_b, pw_b, rw_b, ws_s, ws_r)
    mid_b[c, y] = (hid_b[...].astype(F32) + total).astype(BF16).astype(F32)

    started = [rcopy(mid_b.at[c, y], mid_b.at[c, y], cs_s.at[0], cs_r.at[y], partner)]
    for k in range(1, ny):
        yy = (y + k) % ny
        started.append(rcopy(mid_b.at[c, y], mid_b.at[c, y], ms_s.at[k], ms_r.at[y], peer(yy, x)))
    for cp in started:
        cp.start()
    for cp in col_loads(5):
        cp.start(priority=1)
    for cp in col_loads(6):
        cp.start(priority=1)
    for k in range(1, ny):
        yy = (y + k) % ny
        rcopy(mid_b.at[c, yy], mid_b.at[c, yy], ms_s.at[k], ms_r.at[yy], peer(yy, x)).wait_recv()
        cp = rcopy(mid_b.at[c, yy], mid_b.at[c, yy], cs_s.at[k], cs_r.at[yy], partner)
        cp.start()
        started.append(cp)
    for k in range(ny):
        yy = (y + k) % ny
        rcopy(mid_b.at[oc, yy], mid_b.at[oc, yy], cs_s.at[k], cs_r.at[yy], partner).wait_recv()
    sq = jnp.zeros((xr, 1), F32)
    for ci in range(CORES):
        for yi in range(ny):
            v = mid_b[ci, yi]
            sq = sq + jnp.sum(v * v, axis=-1, keepdims=True)
    inv = lax.rsqrt(sq / width + NORM_EPS)
    g_rows = gain_b[...].astype(F32)
    for ci in range(CORES):
        for yi in range(ny):
            o = ci * hw + yi * cw
            for j in range(cw // LANES):
                row = o // LANES + j
                u2_b[:, o + j * LANES:o + (j + 1) * LANES] = (mid_b[ci, yi, :, j * LANES:(j + 1) * LANES] * inv * g_rows[row:row + 1, :]).astype(BF16)
    for cp in started:
        cp.wait_send()


    def gate_up(j, _):
        for cp in col_loads(j):
            cp.wait()
        lhs = u2_b[...]
        gp = dot32(lhs, wg_b[j])
        up = dot32(lhs, wu_b[j])
        act_b[c, j] = (gp * jax.nn.sigmoid(gp) * up).astype(BF16).astype(F32)
        rcopy(act_b.at[c, j], act_b.at[c, j], dn_s.at[j], dn_r.at[j], partner).start()
        return 0

    wd_loads[0].start(priority=1)
    wd_loads[1].start(priority=1)
    wd_loads[2].start(priority=1)
    wd_loads[3].start(priority=1)
    wd_loads[4].start(priority=1)
    wd_loads[5].start(priority=1)
    wd_loads[6].start(priority=1)
    lax.fori_loop(0, steps, gate_up, 0)

    def take(j, _):
        rcopy(act_b.at[oc, j], act_b.at[oc, j], dn_s.at[j], dn_r.at[j], partner).wait()
        for ci in range(CORES):
            ab_b[:, pl.ds(pl.multiple_of(ci * inner + j * COLS, COLS), COLS)] = act_b[ci, j].astype(BF16)
        return 0

    lax.fori_loop(0, steps, take, 0)
    for cp in wd_loads:
        cp.wait()
    total = reduce_y(lambda: ab_b[...], wd_b, pd_b, rd_b, fs_s, fs_r)
    fin_b[x, y, c] = (mid_b[c, y] + total).astype(BF16).astype(F32)

    def slot(yy, xx):
        return fin_b.at[xx, yy, c]

    def place(k1, k2):
        return (y + k1 * oc + k2 * c) % ny, (x + k1 * c + k2 * oc) % nx

    started = []

    def spread(k1):
        sy, sx = place(k1, 0)
        for k2 in [2, 1, 3] if nx == 4 else range(1, nx):
            ty, tx = place(0, k2)
            cp = rcopy(slot(sy, sx), slot(sy, sx), fp_s.at[k1, k2], fp_r.at[sx, sy, c], peer(ty, tx))
            cp.start()
            started.append(cp)
        cp = rcopy(slot(sy, sx), slot(sy, sx), fp_s.at[k1, 0], fp_r.at[sx, sy, c], partner)
        cp.start()
        started.append(cp)

    for k1 in [2, 1, 3] if ny == 4 else range(1, ny):
        ty, tx = place(k1, 0)
        cp = rcopy(slot(y, x), slot(y, x), fp_s.at[0, nx + k1], fp_r.at[x, y, c], peer(ty, tx))
        cp.start()
        started.append(cp)
    spread(0)

    def arrived(yy, xx, ci):
        return rcopy(fin_b.at[xx, yy, ci], fin_b.at[xx, yy, ci], fp_s.at[0, 0], fp_r.at[xx, yy, ci], partner)

    for k1 in [1, 3, 2] if ny == 4 else range(1, ny):
        sy, sx = place(k1, 0)
        arrived(sy, sx, c).wait_recv()
        spread(k1)
    for k1 in [0, 1, 3, 2] if ny == 4 else range(ny):
        for k2 in [1, 3, 2] if nx == 4 else range(1, nx):
            sy, sx = place(k1, k2)
            arrived(sy, sx, c).wait_recv()
            cp = rcopy(slot(sy, sx), slot(sy, sx), fp_s.at[k1, nx + ny + k2], fp_r.at[sx, sy, c], partner)
            cp.start()
            started.append(cp)
    for xi in range(nx):
        for yi in range(ny):
            arrived(yi, xi, oc).wait_recv()
    for xi in range(nx):
        for yi in range(ny):
            for ci in range(CORES):
                o = ci * hw + yi * cw
                out[xi * xr:(xi + 1) * xr, o:o + cw] = fin_b[xi, yi, ci].astype(BF16)
    for cp in started:
        cp.wait_send()


def mlp(mesh, hidden, o_part, stats, gain, w_o, w_gate, w_up, w_down):
    rows, width = hidden.shape
    heads, _, dim = o_part.shape
    half_h = heads // CORES
    nx = mesh.shape['sp'] // CORES
    ny = mesh.shape['tp']
    xr = rows // nx
    hw = width // CORES
    cw = hw // ny
    inner = w_gate.shape[1] // CORES
    steps = inner // COLS
    any_spec = pl.BlockSpec(memory_space=pl.ANY)
    dma = pltpu.SemaphoreType.DMA
    return pl.pallas_call(
        functools.partial(mlp_kernel, nx, ny),
        name='exchange_mlp',
        out_shape=jax.ShapeDtypeStruct(hidden.shape, BF16),
        in_specs=[any_spec] * 8,
        out_specs=pl.BlockSpec(memory_space=pltpu.VMEM),
        scratch_shapes=[
            pltpu.VMEM((w_o.shape[0], hw), BF16),
            pltpu.VMEM((steps, width, COLS), BF16),
            pltpu.VMEM((steps, width, COLS), BF16),
            pltpu.VMEM((w_down.shape[0], hw), BF16),
            pltpu.VMEM((xr, cw), BF16),
            pltpu.VMEM((width // LANES, LANES), BF16),
            pltpu.VMEM((heads, rows, dim), F32),
            pltpu.VMEM((CORES, heads, rows), F32),
            pltpu.VMEM((half_h, rows, dim), F32),
            pltpu.VMEM((heads, rows), F32),
            pltpu.VMEM((half_h, rows, dim), F32),
            pltpu.VMEM((heads, rows), F32),
            pltpu.VMEM((nx, half_h, xr, dim), F32),
            pltpu.VMEM((nx, heads, rows), F32),
            pltpu.VMEM((nx, rows, heads), F32),
            pltpu.VMEM((CORES, xr, half_h * dim), F32),
            pltpu.VMEM((ny, xr, cw), F32),
            pltpu.VMEM((ny, xr, cw), F32),
            pltpu.VMEM((CORES, ny, xr, cw), F32),
            pltpu.VMEM((xr, width), BF16),
            pltpu.VMEM((CORES, steps, xr, COLS), F32),
            pltpu.VMEM((xr, CORES * inner), BF16),
            pltpu.VMEM((ny, xr, cw), F32),
            pltpu.VMEM((ny, xr, cw), F32),
            pltpu.VMEM((nx, ny, CORES, xr, cw), F32),
            dma((4,)), dma((4,)), dma((steps,)), dma((steps,)), dma((steps,)),
            dma((2,)), dma((2,)),
            dma((nx, 2)), dma((nx, 2)),
            dma((1,)), dma((1,)),
            dma((ny,)), dma((ny,)),
            dma((ny,)), dma((ny,)),
            dma((ny,)), dma((ny,)),
            dma((steps,)), dma((steps,)),
            dma((ny,)), dma((ny,)),
            dma((ny, 2 * nx + ny)), dma((nx, ny, CORES)),
        ],
        compiler_params=pltpu.CompilerParams(vmem_limit_bytes=VMEM_LIMIT, collective_id=0, has_side_effects=True),
    )(hidden, o_part, stats, gain.reshape(width // LANES, LANES), w_o, w_gate, w_up, w_down)


def solution(mesh):
    cache_spec = P('dp', 'tp', 'sp', None)
    row_spec = P('dp', None)
    col_spec = P(None, 'tp')
    inner_spec = P('tp', None)
    gain_spec = P(None)

    def local_step(hidden, seq_lens, k_cache, v_cache, attn_norm, w_q, w_k, w_v, w_o, mlp_norm, w_gate, w_up, w_down):
        o_part, stats, k_out, v_out = attention(hidden, seq_lens, k_cache, v_cache, attn_norm, w_q, w_k, w_v)
        o_part = o_part.reshape(stats.shape[1], stats.shape[2], k_cache.shape[3])
        hidden_out = mlp(mesh, hidden, o_part, stats, mlp_norm, w_o, w_gate, w_up, w_down)
        return hidden_out, k_out, v_out

    return jax.shard_map(local_step, mesh=mesh, in_specs=(row_spec, P('dp'), cache_spec, cache_spec, gain_spec, col_spec, col_spec, col_spec, inner_spec, gain_spec, col_spec, col_spec, inner_spec), out_specs=(row_spec, cache_spec, cache_spec), check_vma=False)
```

```python
import functools
import jax
import jax.numpy as jnp
from jax import lax
from jax.experimental import pallas as pl
from jax.experimental.pallas import tpu as pltpu
from jax.sharding import PartitionSpec as P

NORM_EPS = 1e-6
MASK_VALUE = -3e38
F32 = jnp.float32
BF16 = jnp.bfloat16
MESH = pl.DeviceIdType.MESH
CORES = 2
COLS = 256
LANES = 128
QCOLS = 256
VMEM_LIMIT = 60_000_000


def dot32(a, b):
    return jnp.dot(a, b, preferred_element_type=F32)


def attn_kernel(lens_in, hid, gain, wq, wk, wv, kc, vc, o_out, st_out, k_out, v_out,
                lens, obuf, hbuf, gbuf, ubuf, wbuf, qbuf, knew, vnew, kbuf, vbuf, pbuf,
                hsem, wsem, kin, vin, kos, vos):
    rows, groups, blk, dim = kc.shape
    heads = wq.shape[1] // dim
    rep = heads // groups
    nq = wq.shape[1] // COLS
    nkv = wk.shape[1] // COLS
    nchunk = kin.shape[0]
    crow = rows // nchunk
    base = lax.axis_index('sp') * blk

    def load(i):
        r = pl.ds(i * crow, crow)
        return (pltpu.make_async_copy(kc.at[r], kbuf.at[r], kin.at[i]),
                pltpu.make_async_copy(vc.at[r], vbuf.at[r], vin.at[i]))

    def store(i):
        r = pl.ds(i * crow, crow)
        return (pltpu.make_async_copy(kbuf.at[r], k_out.at[r], kos.at[i]),
                pltpu.make_async_copy(vbuf.at[r], v_out.at[r], vos.at[i]))

    hcopy = pltpu.make_async_copy(hid, hbuf, hsem.at[0])
    gcopy = pltpu.make_async_copy(gain, gbuf, hsem.at[1])
    lcopy = pltpu.make_async_copy(lens_in, lens, hsem.at[2])
    lcopy.start()
    hcopy.start()
    gcopy.start()
    per = COLS // dim

    def weight(src, j, t):
        return pltpu.make_async_copy(src.at[:, pl.ds(j * COLS, COLS)], wbuf.at[t], wsem.at[t])

    weights = [weight(wk, j, j) for j in range(nkv)] + [weight(wv, j, nkv + j) for j in range(nkv)]
    weights += [weight(wq, j, 2 * nkv + j) for j in range(nq)]
    for cp in weights:
        cp.start()
    issued = 1
    for i in range(issued):
        for cp in load(i):
            cp.start()
    lcopy.wait()
    hcopy.wait()
    gcopy.wait()
    g_rows = gbuf[...].astype(F32)
    for r in range(0, rows, 16):
        wide = hbuf[r:r + 16, :].astype(F32)
        inv = lax.rsqrt(jnp.mean(wide * wide, axis=-1, keepdims=True) + NORM_EPS)
        for j in range(gbuf.shape[0]):
            sl = slice(j * LANES, (j + 1) * LANES)
            ubuf[r:r + 16, sl] = (wide[:, sl] * inv * g_rows[j:j + 1, :]).astype(BF16)

    for t, cp in enumerate(weights):
        cp.wait()
        if issued < nchunk:
            for c2 in load(issued):
                c2.start()
            issued += 1
        res = dot32(ubuf[...], wbuf[t])
        for s in range(per):
            part = res[:, s * dim:(s + 1) * dim]
            if t < nkv:
                knew[t * per + s] = part
            elif t < 2 * nkv:
                vnew[(t - nkv) * per + s] = part
            else:
                qbuf[(t - 2 * nkv) * per + s] = part

    tile_row = lax.broadcasted_iota(jnp.int32, (16, dim), 0)

    def update(i):
        for cp in load(i):
            cp.wait()

        def patch(r, _):
            b = i * crow + r
            off = lens[b] - base
            hit = jnp.logical_and(off >= 0, off < blk)
            offc = jnp.clip(off, 0, blk - 1)
            t16 = pl.multiple_of((offc // 16) * 16, 16)
            want = jnp.where(hit, offc - t16, -1)
            mask = tile_row == want
            for gi in range(groups):
                kt = kbuf[b, gi, pl.ds(t16, 16), :]
                kbuf[b, gi, pl.ds(t16, 16), :] = jnp.where(mask, jnp.broadcast_to(knew[gi, pl.ds(b, 1), :], (16, dim)).astype(BF16), kt)
                vt = vbuf[b, gi, pl.ds(t16, 16), :]
                vbuf[b, gi, pl.ds(t16, 16), :] = jnp.where(mask, jnp.broadcast_to(vnew[gi, pl.ds(b, 1), :], (16, dim)).astype(BF16), vt)
            return 0

        lax.fori_loop(0, crow, patch, 0, unroll=4)
        for cp in store(i):
            cp.start()

    ahead = 2
    for i in range(ahead):
        update(i)

    slot_id = lax.broadcasted_iota(jnp.int32, (blk, rep * crow), 0)
    lane_b = lax.broadcasted_iota(jnp.int32, (1, heads * crow), 1) % crow
    low = lax.broadcasted_iota(jnp.int32, (heads, blk), 0) < rep
    scale = dim ** -0.5
    ms, ls = [], []

    for i in range(nchunk):
        if i + ahead < nchunk:
            update(i + ahead)
        b0 = i * crow
        qt = jnp.concatenate([qbuf[h, b0:b0 + crow, :] for h in range(heads)], axis=0).T
        limit = jnp.zeros((1, heads * crow), jnp.int32)
        for r in range(crow):
            limit = jnp.where(lane_b == r, lens[b0 + r] - base, limit)
        rhs = [jnp.concatenate([jnp.where(lane_b[:, :rep * crow] == r, qt[:, gi * rep * crow:(gi + 1) * rep * crow], 0.0).astype(BF16) for r in range(crow)], axis=0) for gi in range(groups)]
        sts = [dot32(jnp.concatenate([kbuf[b0 + r, gi] for r in range(crow)], axis=1), rhs[gi]) for gi in range(groups)]
        mrow, lrow = [], []
        for gi in range(groups):
            lanes = slice(gi * rep * crow, (gi + 1) * rep * crow)
            s = sts[gi] * scale
            valid = slot_id <= limit[:, lanes]
            s = jnp.where(valid, s, MASK_VALUE)
            m = jnp.max(s, axis=0, keepdims=True)
            p = jnp.where(valid, jnp.exp(s - m), 0.0)
            mrow.append(m)
            lrow.append(jnp.sum(p, axis=0, keepdims=True))
            pbuf[gi * rep * crow:(gi + 1) * rep * crow, :] = p.T
        ms.append(mrow)
        ls.append(lrow)
        for r in range(0, crow, 2):
            lhs = []
            for q in range(2):
                ps = pbuf[pl.ds(r + q, heads, stride=crow), :]
                lhs.append(jnp.concatenate([jnp.where(low, ps, 0.0), jnp.where(low, 0.0, ps)], axis=1))
            vals = jnp.concatenate([vbuf[b0 + r].reshape(groups * blk, dim), vbuf[b0 + r + 1].reshape(groups * blk, dim)], axis=1)
            mix = dot32(jnp.concatenate(lhs, axis=0).astype(BF16), vals)
            obuf[pl.ds(b0 + r, heads, stride=rows), :] = mix[:heads, :dim]
            obuf[pl.ds(b0 + r + 1, heads, stride=rows), :] = mix[heads:, dim:]

    ocopy = pltpu.make_async_copy(obuf, o_out, hsem.at[3])
    ocopy.start()
    half = heads // CORES
    for ci in range(CORES):
        for h in range(half):
            gi, ri = divmod(ci * half + h, rep)
            lanes = slice(ri * crow, (ri + 1) * crow)
            st_out[ci, h:h + 1, :] = jnp.concatenate([mrow[gi][:, lanes] for mrow in ms], axis=1)
            st_out[ci, half + h:half + h + 1, :] = jnp.concatenate([lrow[gi][:, lanes] for lrow in ls], axis=1)

    def drain(i, _):
        for cp in store(i):
            cp.wait()
        return 0

    ocopy.wait()
    lax.fori_loop(0, nchunk, drain, 0)


def attention(hidden, seq_lens, k_cache, v_cache, gain, w_q, w_k, w_v):
    rows, groups, blk, dim = k_cache.shape
    heads = w_q.shape[1] // dim
    width = w_q.shape[0]
    nw = (w_q.shape[1] + w_k.shape[1] + w_v.shape[1]) // COLS
    nchunk = 4
    any_spec = pl.BlockSpec(memory_space=pl.ANY)
    vm = pl.BlockSpec(memory_space=pltpu.VMEM)
    return pl.pallas_call(
        attn_kernel,
        name='block_attention',
        out_shape=(jax.ShapeDtypeStruct((heads * rows, dim), F32),
                   jax.ShapeDtypeStruct((CORES, heads, rows), F32),
                   jax.ShapeDtypeStruct(k_cache.shape, BF16),
                   jax.ShapeDtypeStruct(v_cache.shape, BF16)),
        in_specs=[any_spec] * 8,
        out_specs=(any_spec, vm, any_spec, any_spec),
        scratch_shapes=[
            pltpu.SMEM((rows,), jnp.int32),
            pltpu.VMEM((heads * rows, dim), F32),
            pltpu.VMEM((rows, width), BF16),
            pltpu.VMEM((width // LANES, LANES), BF16),
            pltpu.VMEM((rows, width), BF16),
            pltpu.VMEM((nw, width, COLS), BF16),
            pltpu.VMEM((heads, rows, dim), F32),
            pltpu.VMEM((groups, rows, dim), F32),
            pltpu.VMEM((groups, rows, dim), F32),
            pltpu.VMEM(k_cache.shape, BF16),
            pltpu.VMEM(v_cache.shape, BF16),
            pltpu.VMEM((heads * rows // nchunk, blk), F32),
            pltpu.SemaphoreType.DMA((4,)),
            pltpu.SemaphoreType.DMA((nw,)),
            pltpu.SemaphoreType.DMA((nchunk,)),
            pltpu.SemaphoreType.DMA((nchunk,)),
            pltpu.SemaphoreType.DMA((nchunk,)),
            pltpu.SemaphoreType.DMA((nchunk,)),
        ],
        compiler_params=pltpu.CompilerParams(vmem_limit_bytes=VMEM_LIMIT),
    )(seq_lens, hidden, gain.reshape(width // LANES, LANES), w_q, w_k, w_v, k_cache, v_cache)


def mlp_kernel(nx, ny, hid, o_in, st_in, gain, wo, wg, wu, wd, out,
               wo_b, wg_b, wu_b, wd_b, hid_b, gain_b, gf_b, o_b, st_b, po_b, pst_b, oc_b, cst_b, xo_b, xst_b, tst_b,
               att_b, pw_b, rw_b, mid_b, ss_b, g_acc, u_acc, act_b, ab_b, pd_b, rd_b, fin_b,
               lsem, osem, gsem, usem, dsem, ds_s, ds_r, xs_s, xs_r, as_s, as_r, ws_s, ws_r, ms_s, ms_r, cs_s, ss_s, ss_r,
               dn_s, dn_r, fs_s, fs_r, fp_s, fp_r):
    sp = lax.axis_index('sp')
    y = lax.axis_index('tp')
    x = sp // CORES
    c = sp % CORES
    oc = 1 - c
    half_h, rows, dim = po_b.shape
    xr = rows // nx
    width = gain.shape[0] * LANES
    hw = width // CORES
    cw = hw // ny
    nq, qw = mid_b.shape[2], mid_b.shape[4]
    partner = {'tp': y, 'sp': x * CORES + oc}
    far = [2, 1, 3] if ny == 4 else list(range(1, ny))
    near = [1, 3, 2] if ny == 4 else list(range(1, ny))

    def peer(yy, xx):
        return {'tp': yy, 'sp': xx * CORES + c}

    def cross(yy):
        return {'tp': yy, 'sp': x * CORES + oc}

    def rcopy(src, dst, ssem, rsem, dev):
        return pltpu.make_async_remote_copy(src_ref=src, dst_ref=dst, send_sem=ssem, recv_sem=rsem, device_id=dev, device_id_type=MESH)

    def cols(i, n):
        return pl.ds(pl.multiple_of(i * n, n), n)

    loads = [
        pltpu.make_async_copy(o_in, o_b, lsem.at[0]),
        pltpu.make_async_copy(st_in, st_b, lsem.at[1]),
        pltpu.make_async_copy(hid.at[pl.ds(x * xr, xr), pl.ds(pl.multiple_of(c * hw + y * cw, cw), cw)], hid_b, lsem.at[2]),
        pltpu.make_async_copy(gain, gain_b, lsem.at[3]),
    ]
    for cp in loads:
        cp.start()
    steps = wg_b.shape[0]
    inner = steps * COLS

    def row_load(w, w_b, sem, n, j):
        r = cols(j, w_b.shape[0] // n)
        return pltpu.make_async_copy(w.at[r, cols(c, hw)], w_b.at[r], sem.at[j])

    def col_loads(j):
        r = cols(c * steps + j, COLS)
        return (pltpu.make_async_copy(wg.at[:, r], wg_b.at[j], gsem.at[j]), pltpu.make_async_copy(wu.at[:, r], wu_b.at[j], usem.at[j]))

    wo_loads = [row_load(wo, wo_b, osem, osem.shape[0], j) for j in range(osem.shape[0])]
    wd_loads = [row_load(wd, wd_b, dsem, steps, j) for j in range(steps)]
    gu_plan = [range(0, 3), range(3, 5), range(5, steps)]
    wd_plan = [range(0, 4), range(4, steps)]

    def fetch_gu(stage):
        for j in gu_plan[stage]:
            for cp in col_loads(j):
                cp.start(priority=1)

    def fetch_wd(stage):
        for j in wd_plan[stage]:
            wd_loads[j].start(priority=1)

    for cp in wo_loads:
        cp.start(priority=1)
    fetch_gu(0)

    barrier = pltpu.get_barrier_semaphore()
    pl.semaphore_signal(barrier, inc=1, device_id=partner, device_id_type=MESH)
    for k in range(1, nx):
        pl.semaphore_signal(barrier, inc=1, device_id=peer(y, (x + k) % nx), device_id_type=MESH)
    for k in range(1, ny):
        pl.semaphore_signal(barrier, inc=1, device_id=peer((y + k) % ny, x), device_id_type=MESH)
        pl.semaphore_signal(barrier, inc=1, device_id=cross((y + k) % ny), device_id_type=MESH)
    for cp in loads:
        cp.wait()
    gf_b[...] = gain_b[...].astype(F32)
    pl.semaphore_wait(barrier, 1 + (nx - 1) + 2 * (ny - 1))

    d2d = [rcopy(o_b.at[pl.ds(half_h * oc, half_h)], po_b, ds_s.at[0], ds_r.at[0], partner),
           rcopy(st_b.at[oc], pst_b, ds_s.at[1], ds_r.at[1], partner)]
    for cp in d2d:
        cp.start()
    fetch_gu(1)
    for cp in d2d:
        cp.wait()
    s0 = st_b[c]
    s1 = pst_b[...]
    m0, l0, m1, l1 = s0[:half_h], s0[half_h:], s1[:half_h], s1[half_h:]
    mm = jnp.maximum(m0, m1)
    a0, a1 = jnp.exp(m0 - mm), jnp.exp(m1 - mm)
    cst_b[...] = jnp.concatenate([mm, a0 * l0 + a1 * l1], axis=0)
    tr = jnp.concatenate([a0, a1], axis=0).T
    for h in range(half_h):
        oc_b[h] = o_b[half_h * c + h] * tr[:, h:h + 1] + po_b[h] * tr[:, half_h + h:half_h + h + 1]

    sends = []
    for k in range(1, nx):
        xx = (x + k) % nx
        sends.append(rcopy(cst_b, xst_b.at[x], xs_s.at[k - 1, 0], xs_r.at[x, 0], peer(y, xx)))
        sends.append(rcopy(oc_b.at[:, pl.ds(xx * xr, xr), :], xo_b.at[x], xs_s.at[k - 1, 1], xs_r.at[x, 1], peer(y, xx)))
    for cp in sends:
        cp.start()
    fetch_gu(2)
    tst_b[0] = cst_b[...].T
    for k in range(1, nx):
        xx = (x + k) % nx
        rcopy(cst_b, xst_b.at[xx], xs_s.at[k - 1, 0], xs_r.at[xx, 0], peer(y, xx)).wait_recv()
        tst_b[k] = xst_b[xx].T
    stats = [tst_b[k, pl.ds(x * xr, xr), :] for k in range(nx)]
    mm = stats[0][:, :half_h]
    for k in range(1, nx):
        mm = jnp.maximum(mm, stats[k][:, :half_h])
    alphas = [jnp.exp(st[:, :half_h] - mm) for st in stats]
    total = alphas[0] * stats[0][:, half_h:]
    for k in range(1, nx):
        total = total + alphas[k] * stats[k][:, half_h:]
    for k in range(1, nx):
        xx = (x + k) % nx
        rcopy(oc_b.at[:, pl.ds(xx * xr, xr), :], xo_b.at[xx], xs_s.at[k - 1, 1], xs_r.at[xx, 1], peer(y, xx)).wait_recv()
    for h in range(half_h):
        acc = oc_b[h, pl.ds(x * xr, xr), :] * alphas[0][:, h:h + 1]
        for k in range(1, nx):
            acc = acc + xo_b[(x + k) % nx, h] * alphas[k][:, h:h + 1]
        att_b[c, :, h * dim:(h + 1) * dim] = (acc / total[:, h:h + 1]).astype(BF16).astype(F32)
    swap = rcopy(att_b.at[c], att_b.at[c], as_s.at[0], as_r.at[0], partner)
    swap.start()
    for cp in sends:
        cp.wait_send()
    rcopy(att_b.at[oc], att_b.at[oc], as_s.at[0], as_r.at[0], partner).wait_recv()
    swap.wait_send()

    def unit(yy, q):
        return pl.ds(pl.multiple_of(yy * cw + q * qw, qw), qw)

    def send_unit(send_b, recv_b, s_sem, r_sem, q, k):
        yy = (y + k) % ny
        cp = rcopy(send_b.at[q, yy], recv_b.at[q, y], s_sem.at[q, k], r_sem.at[q, y], peer(yy, x))
        cp.start()
        return cp

    def collect(send_b, recv_b, s_sem, r_sem, q):
        total = send_b[q, y]
        for k in range(1, ny):
            yy = (y + k) % ny
            rcopy(send_b.at[q, yy], recv_b.at[q, yy], s_sem.at[q, k], r_sem.at[q, yy], peer(yy, x)).wait_recv()
            total = total + recv_b[q, yy]
        return total

    for cp in wo_loads:
        cp.wait()
    lhs = jnp.concatenate([att_b[0], att_b[1]], axis=1).astype(BF16)
    started = []
    for q in range(nq):
        for k in far + [0]:
            yy = (y + k) % ny
            pw_b[q, yy] = dot32(lhs, wo_b[:, unit(yy, q)])
            if k:
                started.append(send_unit(pw_b, rw_b, ws_s, ws_r, q, k))
    fetch_wd(0)

    def mid_copy(ci, yy, q, ssem, dev):
        return rcopy(mid_b.at[ci, yy, q], mid_b.at[ci, yy, q], ssem, ms_r.at[ci, yy, q], dev)

    sq = jnp.zeros((xr, 1), F32)
    for q in range(nq):
        piece = (hid_b[:, q * qw:(q + 1) * qw].astype(F32) + collect(pw_b, rw_b, ws_s, ws_r, q)).astype(BF16).astype(F32)
        mid_b[c, y, q] = piece
        sq = sq + jnp.sum(piece * piece, axis=-1, keepdims=True)
        sends = []
        if q == nq - 1:
            wide = jnp.broadcast_to(sq, (xr, LANES))
            ss_b[c, y] = jnp.concatenate([wide] * (LANES // xr), axis=0).T[:ss_b.shape[2]]
            sends.append(rcopy(ss_b.at[c, y], ss_b.at[c, y], ss_s.at[0, 0], ss_r.at[c, y], partner))
            for k in range(1, ny):
                yy = (y + k) % ny
                sends.append(rcopy(ss_b.at[c, y], ss_b.at[c, y], ss_s.at[0, k], ss_r.at[c, y], peer(yy, x)))
                sends.append(rcopy(ss_b.at[c, y], ss_b.at[c, y], ss_s.at[1, k], ss_r.at[c, y], cross(yy)))
        sends.append(mid_copy(c, y, q, cs_s.at[q, 0], partner))
        for k in far:
            sends.append(mid_copy(c, y, q, ms_s.at[q, k], peer((y + k) % ny, x)))
        for cp in sends:
            cp.start()
        started += sends
    fetch_wd(1)

    def ss_wait(ci, yy):
        rcopy(ss_b.at[ci, yy], ss_b.at[ci, yy], ss_s.at[0, 0], ss_r.at[ci, yy], partner).wait_recv()

    ss_wait(oc, y)
    for k in range(1, ny):
        ss_wait(c, (y + k) % ny)
        ss_wait(oc, (y + k) % ny)
    tot = ss_b[0, 0]
    for t in range(1, CORES * ny):
        tot = tot + ss_b[t // ny, t % ny]
    inv = lax.rsqrt(tot.T[:xr, :1] / width + NORM_EPS)
    inv = jnp.broadcast_to(inv, (xr, LANES))

    for j in range(steps):
        for cp in col_loads(j):
            cp.wait()

    def accumulate(ci, yy, first):
        start = ci * hw + yy * cw
        parts = []
        for q in range(nq):
            for j in range(qw // LANES):
                g = gf_b[pl.ds(start // LANES + q * (qw // LANES) + j, 1), :]
                parts.append((mid_b[ci, yy, q, :, j * LANES:(j + 1) * LANES] * inv * g).astype(BF16))
        u = jnp.concatenate(parts, axis=1)
        r = pl.ds(pl.multiple_of(start, cw), cw)
        for j in range(steps):
            gp = dot32(u, wg_b[j, r, :])
            up = dot32(u, wu_b[j, r, :])
            g_acc[j] = gp if first else g_acc[j] + gp
            u_acc[j] = up if first else u_acc[j] + up

    def other(yy):
        for q in range(nq):
            mid_copy(oc, yy, q, cs_s.at[q, 0], partner).wait_recv()

    accumulate(c, y, True)
    other(y)
    accumulate(oc, y, False)

    def gather_step(i, _):
        k = i + (i // 2) * (1 - 2 * (i % 2)) if ny == 4 else i
        yy = (y + k) % ny
        for q in range(nq):
            mid_copy(c, yy, q, ms_s.at[q, 0], partner).wait_recv()
            mid_copy(c, yy, q, cs_s.at[q, k], partner).start()
        accumulate(c, yy, False)
        other(yy)
        accumulate(oc, yy, False)
        return 0

    lax.fori_loop(1, ny, gather_step, 0)
    for k in range(1, ny):
        for q in range(nq):
            mid_copy(c, (y + k) % ny, q, cs_s.at[q, k], partner).wait_send()

    acts = []
    for j in range(steps):
        gp = g_acc[j]
        act = (gp * jax.nn.sigmoid(gp) * u_acc[j]).astype(BF16)
        ab_b[c, :, j * COLS:(j + 1) * COLS] = act
        act_b[c, j] = act.astype(F32)
        cp = rcopy(act_b.at[c, j], act_b.at[c, j], dn_s.at[j], dn_r.at[j], partner)
        cp.start()
        acts.append(cp)
    for cp in started:
        cp.wait_send()

    for cp in wd_loads:
        cp.wait()

    def down(ci, yy, q):
        return dot32(ab_b[ci], wd_b[cols(ci, inner), unit(yy, q)])

    started = []
    for k in far + [0]:
        yy = (y + k) % ny
        pd_b[0, yy] = down(c, yy, 0)
    for j in range(steps):
        rcopy(act_b.at[oc, j], act_b.at[oc, j], dn_s.at[j], dn_r.at[j], partner).wait_recv()
        ab_b[oc, :, j * COLS:(j + 1) * COLS] = act_b[oc, j].astype(BF16)
    for q in range(nq):
        for k in far + [0]:
            yy = (y + k) % ny
            rest = down(oc, yy, q)
            pd_b[q, yy] = (pd_b[q, yy] if q == 0 else down(c, yy, q)) + rest
            if k:
                started.append(send_unit(pd_b, rd_b, fs_s, fs_r, q, k))

    def slot(yy, xx, q):
        return fin_b.at[xx, yy, c, q]

    def place(k1, k2, ci):
        oi = 1 - ci
        return (y + k1 * oi + k2 * ci) % ny, (x + k1 * ci + k2 * oi) % nx

    def fcopy(yy, xx, q, ssem, dev):
        return rcopy(slot(yy, xx, q), slot(yy, xx, q), ssem, fp_r.at[xx, yy, c, q], dev)

    def spread(k1, q):
        sy, sx = place(k1, 0, c)
        for k2 in far:
            ty, tx = place(0, k2, c)
            cp = fcopy(sy, sx, q, fp_s.at[q, k1, k2], peer(ty, tx))
            cp.start()
            started.append(cp)
        cp = fcopy(sy, sx, q, fp_s.at[q, k1, 0], partner)
        cp.start()
        started.append(cp)

    def landed(yy, xx, ci, q):
        rcopy(fin_b.at[xx, yy, ci, q], fin_b.at[xx, yy, ci, q], fp_s.at[0, 0, 0], fp_r.at[xx, yy, ci, q], partner).wait_recv()

    def emit(yy, xx, ci, q):
        r = pl.ds(pl.multiple_of(xx * xr, xr), xr)
        out[r, pl.ds(pl.multiple_of(ci * hw + yy * cw + q * qw, qw), qw)] = fin_b[xx, yy, ci, q].astype(BF16)

    for q in range(nq):
        fin_b[x, y, c, q] = (mid_b[c, y, q] + collect(pd_b, rd_b, fs_s, fs_r, q)).astype(BF16).astype(F32)
        for k1 in far:
            ty, tx = place(k1, 0, c)
            cp = fcopy(y, x, q, fp_s.at[q, 0, nx + k1], peer(ty, tx))
            cp.start()
            started.append(cp)
        spread(0, q)
    for q in range(nq):
        for k1 in near:
            sy, sx = place(k1, 0, c)
            landed(sy, sx, c, q)
            spread(k1, q)
        emit(y, x, c, q)
        for k1 in near:
            emit(*place(k1, 0, c), c, q)
    for q in range(nq):
        for k1 in [0] + near:
            for k2 in near:
                sy, sx = place(k1, k2, c)
                landed(sy, sx, c, q)
                cp = fcopy(sy, sx, q, fp_s.at[q, k1, nx + ny + k2], partner)
                cp.start()
                started.append(cp)
                emit(sy, sx, c, q)
        for k1 in [0] + near:
            for k2 in [0] + near:
                sy, sx = place(k1, k2, oc)
                landed(sy, sx, oc, q)
                emit(sy, sx, oc, q)
    for cp in acts + started:
        cp.wait_send()


def mlp(mesh, hidden, o_part, stats, gain, w_o, w_gate, w_up, w_down):
    rows, width = hidden.shape
    heads, _, dim = o_part.shape
    half_h = heads // CORES
    nx = mesh.shape['sp'] // CORES
    ny = mesh.shape['tp']
    xr = rows // nx
    hw = width // CORES
    cw = hw // ny
    inner = w_gate.shape[1] // CORES
    nq = cw // QCOLS
    steps = inner // COLS
    any_spec = pl.BlockSpec(memory_space=pl.ANY)
    dma = pltpu.SemaphoreType.DMA
    return pl.pallas_call(
        functools.partial(mlp_kernel, nx, ny),
        name='exchange_mlp',
        out_shape=pltpu.VMEM(hidden.shape, BF16),
        in_specs=[any_spec] * 8,
        out_specs=pl.BlockSpec(memory_space=pltpu.VMEM),
        scratch_shapes=[
            pltpu.VMEM((w_o.shape[0], hw), BF16),
            pltpu.VMEM((steps, width, COLS), BF16),
            pltpu.VMEM((steps, width, COLS), BF16),
            pltpu.VMEM((w_down.shape[0], hw), BF16),
            pltpu.VMEM((xr, cw), BF16),
            pltpu.VMEM((width // LANES, LANES), BF16),
            pltpu.VMEM((width // LANES, LANES), F32),
            pltpu.VMEM((heads, rows, dim), F32),
            pltpu.VMEM((CORES, heads, rows), F32),
            pltpu.VMEM((half_h, rows, dim), F32),
            pltpu.VMEM((heads, rows), F32),
            pltpu.VMEM((half_h, rows, dim), F32),
            pltpu.VMEM((heads, rows), F32),
            pltpu.VMEM((nx, half_h, xr, dim), F32),
            pltpu.VMEM((nx, heads, rows), F32),
            pltpu.VMEM((nx, rows, heads), F32),
            pltpu.VMEM((CORES, xr, half_h * dim), F32),
            pltpu.VMEM((nq, ny, xr, QCOLS), F32),
            pltpu.VMEM((nq, ny, xr, QCOLS), F32),
            pltpu.VMEM((CORES, ny, nq, xr, QCOLS), F32),
            pltpu.VMEM((CORES, ny, 8, LANES), F32),
            pltpu.VMEM((steps, xr, COLS), F32),
            pltpu.VMEM((steps, xr, COLS), F32),
            pltpu.VMEM((CORES, steps, xr, COLS), F32),
            pltpu.VMEM((CORES, xr, inner), BF16),
            pltpu.VMEM((nq, ny, xr, QCOLS), F32),
            pltpu.VMEM((nq, ny, xr, QCOLS), F32),
            pltpu.VMEM((nx, ny, CORES, nq, xr, QCOLS), F32),
            dma((4,)), dma((4,)), dma((steps,)), dma((steps,)), dma((steps,)),
            dma((2,)), dma((2,)),
            dma((nx, 2)), dma((nx, 2)),
            dma((1,)), dma((1,)),
            dma((nq, ny)), dma((nq, ny)),
            dma((nq, ny)), dma((CORES, ny, nq)), dma((nq, ny)),
            dma((CORES, ny)), dma((CORES, ny)),
            dma((steps,)), dma((steps,)),
            dma((nq, ny)), dma((nq, ny)),
            dma((nq, ny, 2 * nx + ny)), dma((nx, ny, CORES, nq)),
        ],
        compiler_params=pltpu.CompilerParams(vmem_limit_bytes=VMEM_LIMIT, collective_id=0, has_side_effects=True),
    )(hidden, o_part, stats, gain.reshape(width // LANES, LANES), w_o, w_gate, w_up, w_down)


def solution(mesh):
    cache_spec = P('dp', 'tp', 'sp', None)
    row_spec = P('dp', None)
    col_spec = P(None, 'tp')
    inner_spec = P('tp', None)
    gain_spec = P(None)

    def local_step(hidden, seq_lens, k_cache, v_cache, attn_norm, w_q, w_k, w_v, w_o, mlp_norm, w_gate, w_up, w_down):
        o_part, stats, k_out, v_out = attention(hidden, seq_lens, k_cache, v_cache, attn_norm, w_q, w_k, w_v)
        o_part = o_part.reshape(stats.shape[1], stats.shape[2], k_cache.shape[3])
        hidden_out = mlp(mesh, hidden, o_part, stats, mlp_norm, w_o, w_gate, w_up, w_down)
        return hidden_out, k_out, v_out

    return jax.shard_map(local_step, mesh=mesh, in_specs=(row_spec, P('dp'), cache_spec, cache_spec, gain_spec, col_spec, col_spec, col_spec, inner_spec, gain_spec, col_spec, col_spec, inner_spec), out_specs=(row_spec, cache_spec, cache_spec), check_vma=False)
```

```python
import functools
import jax
import jax.numpy as jnp
from jax import lax
from jax.experimental import pallas as pl
from jax.experimental.pallas import tpu as pltpu
from jax.sharding import PartitionSpec as P

NORM_EPS = 1e-6
MASK_VALUE = -3e38
F32 = jnp.float32
BF16 = jnp.bfloat16
MESH = pl.DeviceIdType.MESH
CORES = 2
COLS = 256
LANES = 128
QCOLS = 256
VMEM_LIMIT = 60_000_000


def dot32(a, b):
    return jnp.dot(a, b, preferred_element_type=F32)


def attn_kernel(lens_in, hid, gain, wq, wk, wv, kc, vc, o_out, st_out, k_out, v_out,
                lens, hbuf, gbuf, ubuf, wbuf, qbuf, knew, vnew, kbuf, vbuf, pbuf,
                hsem, wsem, kin, vin, kos, vos):
    rows, groups, blk, dim = kc.shape
    heads = wq.shape[1] // dim
    rep = heads // groups
    nq = wq.shape[1] // COLS
    nkv = wk.shape[1] // COLS
    nchunk = kin.shape[0]
    crow = rows // nchunk
    base = lax.axis_index('sp') * blk

    def load(i):
        r = pl.ds(i * crow, crow)
        return (pltpu.make_async_copy(kc.at[r], kbuf.at[r], kin.at[i]),
                pltpu.make_async_copy(vc.at[r], vbuf.at[r], vin.at[i]))

    def store(i):
        r = pl.ds(i * crow, crow)
        return (pltpu.make_async_copy(kbuf.at[r], k_out.at[r], kos.at[i]),
                pltpu.make_async_copy(vbuf.at[r], v_out.at[r], vos.at[i]))

    hcopy = pltpu.make_async_copy(hid, hbuf, hsem.at[0])
    gcopy = pltpu.make_async_copy(gain, gbuf, hsem.at[1])
    lcopy = pltpu.make_async_copy(lens_in, lens, hsem.at[2])
    lcopy.start()
    hcopy.start()
    gcopy.start()
    per = COLS // dim

    def weight(src, j, t):
        return pltpu.make_async_copy(src.at[:, pl.ds(j * COLS, COLS)], wbuf.at[t], wsem.at[t])

    weights = [weight(wk, j, j) for j in range(nkv)] + [weight(wv, j, nkv + j) for j in range(nkv)]
    weights += [weight(wq, j, 2 * nkv + j) for j in range(nq)]
    for cp in weights:
        cp.start()
    issued = 1
    for i in range(issued):
        for cp in load(i):
            cp.start()
    lcopy.wait()
    hcopy.wait()
    gcopy.wait()
    g_rows = gbuf[...].astype(F32)
    for r in range(0, rows, 16):
        wide = hbuf[r:r + 16, :].astype(F32)
        inv = lax.rsqrt(jnp.mean(wide * wide, axis=-1, keepdims=True) + NORM_EPS)
        for j in range(gbuf.shape[0]):
            sl = slice(j * LANES, (j + 1) * LANES)
            ubuf[r:r + 16, sl] = (wide[:, sl] * inv * g_rows[j:j + 1, :]).astype(BF16)

    for t, cp in enumerate(weights):
        cp.wait()
        if issued < nchunk:
            for c2 in load(issued):
                c2.start()
            issued += 1
        res = dot32(ubuf[...], wbuf[t])
        for s in range(per):
            part = res[:, s * dim:(s + 1) * dim]
            if t < nkv:
                knew[t * per + s] = part
            elif t < 2 * nkv:
                vnew[(t - nkv) * per + s] = part
            else:
                qbuf[(t - 2 * nkv) * per + s] = part

    tile_row = lax.broadcasted_iota(jnp.int32, (16, dim), 0)

    def update(i):
        for cp in load(i):
            cp.wait()

        def patch(r, _):
            b = i * crow + r
            off = lens[b] - base
            hit = jnp.logical_and(off >= 0, off < blk)
            offc = jnp.clip(off, 0, blk - 1)
            t16 = pl.multiple_of((offc // 16) * 16, 16)
            want = jnp.where(hit, offc - t16, -1)
            mask = tile_row == want
            for gi in range(groups):
                kt = kbuf[b, gi, pl.ds(t16, 16), :]
                kbuf[b, gi, pl.ds(t16, 16), :] = jnp.where(mask, jnp.broadcast_to(knew[gi, pl.ds(b, 1), :], (16, dim)).astype(BF16), kt)
                vt = vbuf[b, gi, pl.ds(t16, 16), :]
                vbuf[b, gi, pl.ds(t16, 16), :] = jnp.where(mask, jnp.broadcast_to(vnew[gi, pl.ds(b, 1), :], (16, dim)).astype(BF16), vt)
            return 0

        lax.fori_loop(0, crow, patch, 0, unroll=4)
        for cp in store(i):
            cp.start()

    ahead = 2
    for i in range(ahead):
        update(i)

    slot_id = lax.broadcasted_iota(jnp.int32, (blk, rep * crow), 0)
    lane_b = lax.broadcasted_iota(jnp.int32, (1, heads * crow), 1) % crow
    low = lax.broadcasted_iota(jnp.int32, (heads, blk), 0) < rep
    scale = dim ** -0.5
    ms, ls = [], []

    for i in range(nchunk):
        if i + ahead < nchunk:
            update(i + ahead)
        b0 = i * crow
        qt = jnp.concatenate([qbuf[h, b0:b0 + crow, :] for h in range(heads)], axis=0).T
        limit = jnp.zeros((1, heads * crow), jnp.int32)
        for r in range(crow):
            limit = jnp.where(lane_b == r, lens[b0 + r] - base, limit)
        rhs = [jnp.concatenate([jnp.where(lane_b[:, :rep * crow] == r, qt[:, gi * rep * crow:(gi + 1) * rep * crow], 0.0).astype(BF16) for r in range(crow)], axis=0) for gi in range(groups)]
        sts = [dot32(jnp.concatenate([kbuf[b0 + r, gi] for r in range(crow)], axis=1), rhs[gi]) for gi in range(groups)]
        mrow, lrow = [], []
        for gi in range(groups):
            lanes = slice(gi * rep * crow, (gi + 1) * rep * crow)
            s = sts[gi] * scale
            valid = slot_id <= limit[:, lanes]
            s = jnp.where(valid, s, MASK_VALUE)
            m = jnp.max(s, axis=0, keepdims=True)
            p = jnp.where(valid, jnp.exp(s - m), 0.0)
            mrow.append(m)
            lrow.append(jnp.sum(p, axis=0, keepdims=True))
            pbuf[gi * rep * crow:(gi + 1) * rep * crow, :] = p.T
        ms.append(mrow)
        ls.append(lrow)
        for r in range(0, crow, 2):
            lhs = []
            for q in range(2):
                ps = pbuf[pl.ds(r + q, heads, stride=crow), :]
                lhs.append(jnp.concatenate([jnp.where(low, ps, 0.0), jnp.where(low, 0.0, ps)], axis=1))
            vals = jnp.concatenate([vbuf[b0 + r].reshape(groups * blk, dim), vbuf[b0 + r + 1].reshape(groups * blk, dim)], axis=1)
            mix = dot32(jnp.concatenate(lhs, axis=0).astype(BF16), vals)
            o_out[pl.ds(b0 + r, heads, stride=rows), :] = mix[:heads, :dim]
            o_out[pl.ds(b0 + r + 1, heads, stride=rows), :] = mix[heads:, dim:]

    half = heads // CORES
    for ci in range(CORES):
        for h in range(half):
            gi, ri = divmod(ci * half + h, rep)
            lanes = slice(ri * crow, (ri + 1) * crow)
            st_out[ci, h:h + 1, :] = jnp.concatenate([mrow[gi][:, lanes] for mrow in ms], axis=1)
            st_out[ci, half + h:half + h + 1, :] = jnp.concatenate([lrow[gi][:, lanes] for lrow in ls], axis=1)

    def drain(i, _):
        for cp in store(i):
            cp.wait()
        return 0

    lax.fori_loop(0, nchunk, drain, 0)


def attention(hidden, seq_lens, k_cache, v_cache, gain, w_q, w_k, w_v):
    rows, groups, blk, dim = k_cache.shape
    heads = w_q.shape[1] // dim
    width = w_q.shape[0]
    nw = (w_q.shape[1] + w_k.shape[1] + w_v.shape[1]) // COLS
    nchunk = 4
    any_spec = pl.BlockSpec(memory_space=pl.ANY)
    vm = pl.BlockSpec(memory_space=pltpu.VMEM)
    return pl.pallas_call(
        attn_kernel,
        name='block_attention',
        out_shape=(pltpu.VMEM((heads * rows, dim), F32),
                   pltpu.VMEM((CORES, heads, rows), F32),
                   jax.ShapeDtypeStruct(k_cache.shape, BF16),
                   jax.ShapeDtypeStruct(v_cache.shape, BF16)),
        in_specs=[any_spec] * 8,
        out_specs=(vm, vm, any_spec, any_spec),
        scratch_shapes=[
            pltpu.SMEM((rows,), jnp.int32),
            pltpu.VMEM((rows, width), BF16),
            pltpu.VMEM((width // LANES, LANES), BF16),
            pltpu.VMEM((rows, width), BF16),
            pltpu.VMEM((nw, width, COLS), BF16),
            pltpu.VMEM((heads, rows, dim), F32),
            pltpu.VMEM((groups, rows, dim), F32),
            pltpu.VMEM((groups, rows, dim), F32),
            pltpu.VMEM(k_cache.shape, BF16),
            pltpu.VMEM(v_cache.shape, BF16),
            pltpu.VMEM((heads * rows // nchunk, blk), F32),
            pltpu.SemaphoreType.DMA((4,)),
            pltpu.SemaphoreType.DMA((nw,)),
            pltpu.SemaphoreType.DMA((nchunk,)),
            pltpu.SemaphoreType.DMA((nchunk,)),
            pltpu.SemaphoreType.DMA((nchunk,)),
            pltpu.SemaphoreType.DMA((nchunk,)),
        ],
        compiler_params=pltpu.CompilerParams(vmem_limit_bytes=VMEM_LIMIT),
    )(seq_lens, hidden, gain.reshape(width // LANES, LANES), w_q, w_k, w_v, k_cache, v_cache)


def mlp_kernel(nx, ny, hid, o_b, st_b, gain, wo, wg, wu, wd, out,
               wo_b, wg_b, wu_b, wd_b, hid_b, gain_b, gf_b, po_b, pst_b, oc_b, cst_b, xo_b, xst_b, tst_b,
               att_b, pw_b, rw_b, mid_b, ss_b, g_acc, u_acc, act_b, ab_b, pd_b, rd_b, fin_b,
               lsem, osem, gsem, usem, dsem, ds_s, ds_r, xs_s, xs_r, as_s, as_r, ws_s, ws_r, ms_s, ms_r, cs_s, ss_s, ss_r,
               dn_s, dn_r, fs_s, fs_r, fp_s, fp_r):
    sp = lax.axis_index('sp')
    y = lax.axis_index('tp')
    x = sp // CORES
    c = sp % CORES
    oc = 1 - c
    half_h, rows, dim = po_b.shape
    xr = rows // nx
    width = gain.shape[0] * LANES
    hw = width // CORES
    cw = hw // ny
    nq, qw = mid_b.shape[2], mid_b.shape[4]
    partner = {'tp': y, 'sp': x * CORES + oc}
    far = [2, 1, 3] if ny == 4 else list(range(1, ny))
    near = [1, 3, 2] if ny == 4 else list(range(1, ny))

    def peer(yy, xx):
        return {'tp': yy, 'sp': xx * CORES + c}

    def cross(yy):
        return {'tp': yy, 'sp': x * CORES + oc}

    def rcopy(src, dst, ssem, rsem, dev):
        return pltpu.make_async_remote_copy(src_ref=src, dst_ref=dst, send_sem=ssem, recv_sem=rsem, device_id=dev, device_id_type=MESH)

    def cols(i, n):
        return pl.ds(pl.multiple_of(i * n, n), n)

    loads = [
        pltpu.make_async_copy(hid.at[pl.ds(x * xr, xr), pl.ds(pl.multiple_of(c * hw + y * cw, cw), cw)], hid_b, lsem.at[2]),
        pltpu.make_async_copy(gain, gain_b, lsem.at[3]),
    ]
    for cp in loads:
        cp.start()
    steps = wg_b.shape[0]
    inner = steps * COLS

    def row_load(w, w_b, sem, n, j):
        r = cols(j, w_b.shape[0] // n)
        return pltpu.make_async_copy(w.at[r, cols(c, hw)], w_b.at[r], sem.at[j])

    def col_loads(j):
        r = cols(c * steps + j, COLS)
        return (pltpu.make_async_copy(wg.at[:, r], wg_b.at[j], gsem.at[j]), pltpu.make_async_copy(wu.at[:, r], wu_b.at[j], usem.at[j]))

    wo_loads = [row_load(wo, wo_b, osem, osem.shape[0], j) for j in range(osem.shape[0])]
    wd_loads = [row_load(wd, wd_b, dsem, steps, j) for j in range(steps)]
    gu_plan = [range(0, 3), range(3, 5), range(5, steps)]
    wd_plan = [range(0, 4), range(4, steps)]

    def fetch_gu(stage):
        for j in gu_plan[stage]:
            for cp in col_loads(j):
                cp.start(priority=1)

    def fetch_wd(stage):
        for j in wd_plan[stage]:
            wd_loads[j].start(priority=1)

    for cp in wo_loads:
        cp.start(priority=1)
    fetch_gu(0)

    barrier = pltpu.get_barrier_semaphore()
    pl.semaphore_signal(barrier, inc=1, device_id=partner, device_id_type=MESH)
    for k in range(1, nx):
        pl.semaphore_signal(barrier, inc=1, device_id=peer(y, (x + k) % nx), device_id_type=MESH)
    for k in range(1, ny):
        pl.semaphore_signal(barrier, inc=1, device_id=peer((y + k) % ny, x), device_id_type=MESH)
        pl.semaphore_signal(barrier, inc=1, device_id=cross((y + k) % ny), device_id_type=MESH)
    pl.semaphore_wait(barrier, 1 + (nx - 1) + 2 * (ny - 1))

    def head_rows(h):
        return pl.ds(pl.multiple_of(h * rows, rows), rows)

    swap = [rcopy(st_b.at[oc], pst_b, ds_s.at[half_h], ds_r.at[half_h], partner)]
    for h in range(half_h):
        swap.append(rcopy(o_b.at[head_rows(half_h * oc + h)], po_b.at[h], ds_s.at[h], ds_r.at[h], partner))
    for cp in swap:
        cp.start()
    fetch_gu(1)
    swap[0].wait_recv()
    s0 = st_b[c]
    s1 = pst_b[...]
    m0, l0, m1, l1 = s0[:half_h], s0[half_h:], s1[:half_h], s1[half_h:]
    mm = jnp.maximum(m0, m1)
    a0, a1 = jnp.exp(m0 - mm), jnp.exp(m1 - mm)
    cst_b[...] = jnp.concatenate([mm, a0 * l0 + a1 * l1], axis=0)

    far_x = [2, 1, 3] if nx == 4 else list(range(1, nx))
    sends = []
    for k in far_x:
        sends.append(rcopy(cst_b, xst_b.at[x], xs_s.at[k - 1, half_h], xs_r.at[x, half_h], peer(y, (x + k) % nx)))
    for cp in sends:
        cp.start()
    tr = jnp.concatenate([a0, a1], axis=0).T
    for h in range(half_h):
        swap[1 + h].wait_recv()
        oc_b[h] = o_b[head_rows(half_h * c + h), :] * tr[:, h:h + 1] + po_b[h] * tr[:, half_h + h:half_h + h + 1]
        for k in far_x:
            xx = (x + k) % nx
            cp = rcopy(oc_b.at[h, pl.ds(xx * xr, xr), :], xo_b.at[x, h], xs_s.at[k - 1, h], xs_r.at[x, h], peer(y, xx))
            cp.start()
            sends.append(cp)
    fetch_gu(2)
    tst_b[0] = cst_b[...].T
    for k in range(1, nx):
        xx = (x + k) % nx
        rcopy(cst_b, xst_b.at[xx], xs_s.at[k - 1, half_h], xs_r.at[xx, half_h], peer(y, xx)).wait_recv()
        tst_b[k] = xst_b[xx].T
    stats = [tst_b[k, pl.ds(x * xr, xr), :] for k in range(nx)]
    mm = stats[0][:, :half_h]
    for k in range(1, nx):
        mm = jnp.maximum(mm, stats[k][:, :half_h])
    alphas = [jnp.exp(st[:, :half_h] - mm) for st in stats]
    total = alphas[0] * stats[0][:, half_h:]
    for k in range(1, nx):
        total = total + alphas[k] * stats[k][:, half_h:]
    for h in range(half_h):
        acc = oc_b[h, pl.ds(x * xr, xr), :] * alphas[0][:, h:h + 1]
        for k in range(1, nx):
            xx = (x + k) % nx
            rcopy(oc_b.at[h, pl.ds(xx * xr, xr), :], xo_b.at[xx, h], xs_s.at[k - 1, h], xs_r.at[xx, h], peer(y, xx)).wait_recv()
            acc = acc + xo_b[xx, h] * alphas[k][:, h:h + 1]
        att_b[c, h] = (acc / total[:, h:h + 1]).astype(BF16).astype(F32)
        cp = rcopy(att_b.at[c, h], att_b.at[c, h], as_s.at[h], as_r.at[h], partner)
        cp.start()
        sends.append(cp)

    def unit(yy, q):
        return pl.ds(pl.multiple_of(yy * cw + q * qw, qw), qw)

    def send_unit(send_b, recv_b, s_sem, r_sem, q, k):
        yy = (y + k) % ny
        cp = rcopy(send_b.at[q, yy], recv_b.at[q, y], s_sem.at[q, k], r_sem.at[q, y], peer(yy, x))
        cp.start()
        return cp

    def collect(send_b, recv_b, s_sem, r_sem, q):
        total = send_b[q, y]
        for k in range(1, ny):
            yy = (y + k) % ny
            rcopy(send_b.at[q, yy], recv_b.at[q, yy], s_sem.at[q, k], r_sem.at[q, yy], peer(yy, x)).wait_recv()
            total = total + recv_b[q, yy]
        return total

    for cp in loads:
        cp.wait()
    gf_b[...] = gain_b[...].astype(F32)

    for cp in wo_loads:
        cp.wait()
    started = swap + sends

    def attended(ci):
        return jnp.concatenate([att_b[ci, h] for h in range(half_h)], axis=1).astype(BF16)

    own_att = attended(c)
    for q in range(nq):
        for k in far + [0]:
            yy = (y + k) % ny
            pw_b[q, yy] = dot32(own_att, wo_b[cols(c, half_h * dim), unit(yy, q)])
    for h in range(half_h):
        rcopy(att_b.at[oc, h], att_b.at[oc, h], as_s.at[h], as_r.at[h], partner).wait_recv()
    other_att = attended(oc)
    for q in range(nq):
        for k in far + [0]:
            yy = (y + k) % ny
            pw_b[q, yy] = pw_b[q, yy] + dot32(other_att, wo_b[cols(oc, half_h * dim), unit(yy, q)])
            if k:
                started.append(send_unit(pw_b, rw_b, ws_s, ws_r, q, k))
    fetch_wd(0)

    def mid_copy(ci, yy, q, ssem, dev):
        return rcopy(mid_b.at[ci, yy, q], mid_b.at[ci, yy, q], ssem, ms_r.at[ci, yy, q], dev)

    sq = jnp.zeros((xr, 1), F32)
    for q in range(nq):
        piece = (hid_b[:, q * qw:(q + 1) * qw].astype(F32) + collect(pw_b, rw_b, ws_s, ws_r, q)).astype(BF16).astype(F32)
        mid_b[c, y, q] = piece
        sq = sq + jnp.sum(piece * piece, axis=-1, keepdims=True)
        sends = []
        if q == nq - 1:
            wide = jnp.broadcast_to(sq, (xr, LANES))
            ss_b[c, y] = jnp.concatenate([wide] * (LANES // xr), axis=0).T[:ss_b.shape[2]]
            sends.append(rcopy(ss_b.at[c, y], ss_b.at[c, y], ss_s.at[0, 0], ss_r.at[c, y], partner))
            for k in range(1, ny):
                yy = (y + k) % ny
                sends.append(rcopy(ss_b.at[c, y], ss_b.at[c, y], ss_s.at[0, k], ss_r.at[c, y], peer(yy, x)))
                sends.append(rcopy(ss_b.at[c, y], ss_b.at[c, y], ss_s.at[1, k], ss_r.at[c, y], cross(yy)))
        sends.append(mid_copy(c, y, q, cs_s.at[q, 0], partner))
        for k in far:
            sends.append(mid_copy(c, y, q, ms_s.at[q, k], peer((y + k) % ny, x)))
        for cp in sends:
            cp.start()
        started += sends
    fetch_wd(1)

    def ss_wait(ci, yy):
        rcopy(ss_b.at[ci, yy], ss_b.at[ci, yy], ss_s.at[0, 0], ss_r.at[ci, yy], partner).wait_recv()

    ss_wait(oc, y)
    for k in range(1, ny):
        ss_wait(c, (y + k) % ny)
        ss_wait(oc, (y + k) % ny)
    tot = ss_b[0, 0]
    for t in range(1, CORES * ny):
        tot = tot + ss_b[t // ny, t % ny]
    inv = lax.rsqrt(tot.T[:xr, :1] / width + NORM_EPS)
    inv = jnp.broadcast_to(inv, (xr, LANES))

    for j in range(steps):
        for cp in col_loads(j):
            cp.wait()

    def accumulate(ci, yy, first):
        start = ci * hw + yy * cw
        parts = []
        for q in range(nq):
            for j in range(qw // LANES):
                g = gf_b[pl.ds(start // LANES + q * (qw // LANES) + j, 1), :]
                parts.append((mid_b[ci, yy, q, :, j * LANES:(j + 1) * LANES] * inv * g).astype(BF16))
        u = jnp.concatenate(parts, axis=1)
        r = pl.ds(pl.multiple_of(start, cw), cw)
        for j in range(steps):
            gp = dot32(u, wg_b[j, r, :])
            up = dot32(u, wu_b[j, r, :])
            g_acc[j] = gp if first else g_acc[j] + gp
            u_acc[j] = up if first else u_acc[j] + up

    def other(yy):
        for q in range(nq):
            mid_copy(oc, yy, q, cs_s.at[q, 0], partner).wait_recv()

    accumulate(c, y, True)
    other(y)
    accumulate(oc, y, False)

    def gather_step(i, _):
        k = i + (i // 2) * (1 - 2 * (i % 2)) if ny == 4 else i
        yy = (y + k) % ny
        for q in range(nq):
            mid_copy(c, yy, q, ms_s.at[q, 0], partner).wait_recv()
            mid_copy(c, yy, q, cs_s.at[q, k], partner).start()
        accumulate(c, yy, False)
        other(yy)
        accumulate(oc, yy, False)
        return 0

    lax.fori_loop(1, ny, gather_step, 0)
    for k in range(1, ny):
        for q in range(nq):
            mid_copy(c, (y + k) % ny, q, cs_s.at[q, k], partner).wait_send()

    acts = []
    for j in range(steps):
        gp = g_acc[j]
        act = (gp * jax.nn.sigmoid(gp) * u_acc[j]).astype(BF16)
        ab_b[c, :, j * COLS:(j + 1) * COLS] = act
        act_b[c, j] = act.astype(F32)
        cp = rcopy(act_b.at[c, j], act_b.at[c, j], dn_s.at[j], dn_r.at[j], partner)
        cp.start()
        acts.append(cp)
    for cp in started:
        cp.wait_send()

    for cp in wd_loads:
        cp.wait()

    def down(ci, yy, q):
        return dot32(ab_b[ci], wd_b[cols(ci, inner), unit(yy, q)])

    started = []
    for k in far + [0]:
        yy = (y + k) % ny
        pd_b[0, yy] = down(c, yy, 0)
    for j in range(steps):
        rcopy(act_b.at[oc, j], act_b.at[oc, j], dn_s.at[j], dn_r.at[j], partner).wait_recv()
        ab_b[oc, :, j * COLS:(j + 1) * COLS] = act_b[oc, j].astype(BF16)
    for q in range(nq):
        for k in far + [0]:
            yy = (y + k) % ny
            rest = down(oc, yy, q)
            pd_b[q, yy] = (pd_b[q, yy] if q == 0 else down(c, yy, q)) + rest
            if k:
                started.append(send_unit(pd_b, rd_b, fs_s, fs_r, q, k))

    def slot(yy, xx, q):
        return fin_b.at[xx, yy, c, q]

    def place(k1, k2, ci):
        oi = 1 - ci
        return (y + k1 * oi + k2 * ci) % ny, (x + k1 * ci + k2 * oi) % nx

    def fcopy(yy, xx, q, ssem, dev):
        return rcopy(slot(yy, xx, q), slot(yy, xx, q), ssem, fp_r.at[xx, yy, c, q], dev)

    def spread(k1, q):
        sy, sx = place(k1, 0, c)
        for k2 in far_x:
            ty, tx = place(0, k2, c)
            cp = fcopy(sy, sx, q, fp_s.at[q, k1, k2], peer(ty, tx))
            cp.start()
            started.append(cp)
        cp = fcopy(sy, sx, q, fp_s.at[q, k1, 0], partner)
        cp.start()
        started.append(cp)

    def landed(yy, xx, ci, q):
        rcopy(fin_b.at[xx, yy, ci, q], fin_b.at[xx, yy, ci, q], fp_s.at[0, 0, 0], fp_r.at[xx, yy, ci, q], partner).wait_recv()

    def emit(yy, xx, ci, q):
        r = pl.ds(pl.multiple_of(xx * xr, xr), xr)
        out[r, pl.ds(pl.multiple_of(ci * hw + yy * cw + q * qw, qw), qw)] = fin_b[xx, yy, ci, q].astype(BF16)

    for q in range(nq):
        fin_b[x, y, c, q] = (mid_b[c, y, q] + collect(pd_b, rd_b, fs_s, fs_r, q)).astype(BF16).astype(F32)
        for k1 in far:
            ty, tx = place(k1, 0, c)
            cp = fcopy(y, x, q, fp_s.at[q, 0, nx + k1], peer(ty, tx))
            cp.start()
            started.append(cp)
        spread(0, q)
    for q in range(nq):
        for k1 in near:
            sy, sx = place(k1, 0, c)
            landed(sy, sx, c, q)
            spread(k1, q)
        emit(y, x, c, q)
        for k1 in near:
            emit(*place(k1, 0, c), c, q)
    order = [(k1, k2) for k1 in [0] + near for k2 in near]
    for q in range(nq):
        for k1, k2 in order:
            sy, sx = place(k1, k2, c)
            landed(sy, sx, c, q)
            cp = fcopy(sy, sx, q, fp_s.at[q, k1, nx + ny + k2], partner)
            cp.start()
            started.append(cp)
            emit(sy, sx, c, q)
    for q in range(nq):
        for k1, k2 in [(k1, 0) for k1 in [0] + near] + order:
            sy, sx = place(k1, k2, oc)
            landed(sy, sx, oc, q)
            emit(sy, sx, oc, q)
    for cp in acts + started:
        cp.wait_send()


def mlp(mesh, hidden, o_part, stats, gain, w_o, w_gate, w_up, w_down):
    rows, width = hidden.shape
    heads = stats.shape[1]
    dim = o_part.shape[1]
    half_h = heads // CORES
    nx = mesh.shape['sp'] // CORES
    ny = mesh.shape['tp']
    xr = rows // nx
    hw = width // CORES
    cw = hw // ny
    inner = w_gate.shape[1] // CORES
    nq = cw // QCOLS
    steps = inner // COLS
    any_spec = pl.BlockSpec(memory_space=pl.ANY)
    vm = pl.BlockSpec(memory_space=pltpu.VMEM)
    dma = pltpu.SemaphoreType.DMA
    return pl.pallas_call(
        functools.partial(mlp_kernel, nx, ny),
        name='exchange_mlp',
        out_shape=pltpu.VMEM(hidden.shape, BF16),
        in_specs=[any_spec, vm, vm] + [any_spec] * 5,
        out_specs=vm,
        scratch_shapes=[
            pltpu.VMEM((w_o.shape[0], hw), BF16),
            pltpu.VMEM((steps, width, COLS), BF16),
            pltpu.VMEM((steps, width, COLS), BF16),
            pltpu.VMEM((w_down.shape[0], hw), BF16),
            pltpu.VMEM((xr, cw), BF16),
            pltpu.VMEM((width // LANES, LANES), BF16),
            pltpu.VMEM((width // LANES, LANES), F32),
            pltpu.VMEM((half_h, rows, dim), F32),
            pltpu.VMEM((heads, rows), F32),
            pltpu.VMEM((half_h, rows, dim), F32),
            pltpu.VMEM((heads, rows), F32),
            pltpu.VMEM((nx, half_h, xr, dim), F32),
            pltpu.VMEM((nx, heads, rows), F32),
            pltpu.VMEM((nx, rows, heads), F32),
            pltpu.VMEM((CORES, half_h, xr, dim), F32),
            pltpu.VMEM((nq, ny, xr, QCOLS), F32),
            pltpu.VMEM((nq, ny, xr, QCOLS), F32),
            pltpu.VMEM((CORES, ny, nq, xr, QCOLS), F32),
            pltpu.VMEM((CORES, ny, 8, LANES), F32),
            pltpu.VMEM((steps, xr, COLS), F32),
            pltpu.VMEM((steps, xr, COLS), F32),
            pltpu.VMEM((CORES, steps, xr, COLS), F32),
            pltpu.VMEM((CORES, xr, inner), BF16),
            pltpu.VMEM((nq, ny, xr, QCOLS), F32),
            pltpu.VMEM((nq, ny, xr, QCOLS), F32),
            pltpu.VMEM((nx, ny, CORES, nq, xr, QCOLS), F32),
            dma((4,)), dma((4,)), dma((steps,)), dma((steps,)), dma((steps,)),
            dma((half_h + 1,)), dma((half_h + 1,)),
            dma((nx, half_h + 1)), dma((nx, half_h + 1)),
            dma((half_h,)), dma((half_h,)),
            dma((nq, ny)), dma((nq, ny)),
            dma((nq, ny)), dma((CORES, ny, nq)), dma((nq, ny)),
            dma((CORES, ny)), dma((CORES, ny)),
            dma((steps,)), dma((steps,)),
            dma((nq, ny)), dma((nq, ny)),
            dma((nq, ny, 2 * nx + ny)), dma((nx, ny, CORES, nq)),
        ],
        compiler_params=pltpu.CompilerParams(vmem_limit_bytes=VMEM_LIMIT, collective_id=0, has_side_effects=True),
    )(hidden, pltpu.with_memory_space_constraint(o_part, pltpu.VMEM), pltpu.with_memory_space_constraint(stats, pltpu.VMEM), gain.reshape(width // LANES, LANES), w_o, w_gate, w_up, w_down)


def solution(mesh):
    cache_spec = P('dp', 'tp', 'sp', None)
    row_spec = P('dp', None)
    col_spec = P(None, 'tp')
    inner_spec = P('tp', None)
    gain_spec = P(None)

    def local_step(hidden, seq_lens, k_cache, v_cache, attn_norm, w_q, w_k, w_v, w_o, mlp_norm, w_gate, w_up, w_down):
        o_part, stats, k_out, v_out = attention(hidden, seq_lens, k_cache, v_cache, attn_norm, w_q, w_k, w_v)
        hidden_out = mlp(mesh, hidden, o_part, stats, mlp_norm, w_o, w_gate, w_up, w_down)
        return hidden_out, k_out, v_out

    return jax.shard_map(local_step, mesh=mesh, in_specs=(row_spec, P('dp'), cache_spec, cache_spec, gain_spec, col_spec, col_spec, col_spec, inner_spec, gain_spec, col_spec, col_spec, inner_spec), out_specs=(row_spec, cache_spec, cache_spec), check_vma=False)
```

```python
import functools
import jax
import jax.numpy as jnp
from jax import lax
from jax.experimental import pallas as pl
from jax.experimental.pallas import tpu as pltpu
from jax.sharding import PartitionSpec as P

NORM_EPS = 1e-6
MASK_VALUE = -3e38
F32 = jnp.float32
BF16 = jnp.bfloat16
MESH = pl.DeviceIdType.MESH
CORES = 2
COLS = 256
LANES = 128
QCOLS = 256
VMEM_LIMIT = 60_000_000


def dot32(a, b):
    return jnp.dot(a, b, preferred_element_type=F32)


def attn_kernel(lens_in, hid, gain, wq, wk, wv, kc, vc, o_out, st_out, k_out, v_out,
                lens, hbuf, gbuf, ubuf, wbuf, qbuf, knew, vnew, kbuf, vbuf, pbuf,
                hsem, wsem, kin, vin, kos, vos):
    rows, groups, blk, dim = kc.shape
    heads = wq.shape[1] // dim
    rep = heads // groups
    nq = wq.shape[1] // COLS
    nkv = wk.shape[1] // COLS
    nchunk = kin.shape[0]
    crow = rows // nchunk
    base = lax.axis_index('sp') * blk

    def load(i):
        r = pl.ds(i * crow, crow)
        return (pltpu.make_async_copy(kc.at[r], kbuf.at[r], kin.at[i]),
                pltpu.make_async_copy(vc.at[r], vbuf.at[r], vin.at[i]))

    def store(i):
        r = pl.ds(i * crow, crow)
        return (pltpu.make_async_copy(kbuf.at[r], k_out.at[r], kos.at[i]),
                pltpu.make_async_copy(vbuf.at[r], v_out.at[r], vos.at[i]))

    hcopy = pltpu.make_async_copy(hid, hbuf, hsem.at[0])
    gcopy = pltpu.make_async_copy(gain, gbuf, hsem.at[1])
    lcopy = pltpu.make_async_copy(lens_in, lens, hsem.at[2])
    lcopy.start()
    hcopy.start()
    gcopy.start()
    per = COLS // dim

    def weight(src, j, t):
        return pltpu.make_async_copy(src.at[:, pl.ds(j * COLS, COLS)], wbuf.at[t], wsem.at[t])

    weights = [weight(wk, j, j) for j in range(nkv)] + [weight(wv, j, nkv + j) for j in range(nkv)]
    weights += [weight(wq, j, 2 * nkv + j) for j in range(nq)]
    for cp in weights:
        cp.start()
    issued = 1
    for i in range(issued):
        for cp in load(i):
            cp.start()
    lcopy.wait()
    hcopy.wait()
    gcopy.wait()
    g_rows = gbuf[...].astype(F32)
    for r in range(0, rows, 16):
        wide = hbuf[r:r + 16, :].astype(F32)
        inv = lax.rsqrt(jnp.mean(wide * wide, axis=-1, keepdims=True) + NORM_EPS)
        for j in range(gbuf.shape[0]):
            sl = slice(j * LANES, (j + 1) * LANES)
            ubuf[r:r + 16, sl] = (wide[:, sl] * inv * g_rows[j:j + 1, :]).astype(BF16)

    for t, cp in enumerate(weights):
        cp.wait()
        if issued < nchunk:
            for c2 in load(issued):
                c2.start()
            issued += 1
        res = dot32(ubuf[...], wbuf[t])
        for s in range(per):
            part = res[:, s * dim:(s + 1) * dim]
            if t < nkv:
                knew[t * per + s] = part
            elif t < 2 * nkv:
                vnew[(t - nkv) * per + s] = part
            else:
                qbuf[(t - 2 * nkv) * per + s] = part

    tile_row = lax.broadcasted_iota(jnp.int32, (16, dim), 0)

    def update(i):
        for cp in load(i):
            cp.wait()

        def patch(r, _):
            b = i * crow + r
            off = lens[b] - base
            hit = jnp.logical_and(off >= 0, off < blk)
            offc = jnp.clip(off, 0, blk - 1)
            t16 = pl.multiple_of((offc // 16) * 16, 16)
            want = jnp.where(hit, offc - t16, -1)
            mask = tile_row == want
            for gi in range(groups):
                kt = kbuf[b, gi, pl.ds(t16, 16), :]
                kbuf[b, gi, pl.ds(t16, 16), :] = jnp.where(mask, jnp.broadcast_to(knew[gi, pl.ds(b, 1), :], (16, dim)).astype(BF16), kt)
                vt = vbuf[b, gi, pl.ds(t16, 16), :]
                vbuf[b, gi, pl.ds(t16, 16), :] = jnp.where(mask, jnp.broadcast_to(vnew[gi, pl.ds(b, 1), :], (16, dim)).astype(BF16), vt)
            return 0

        lax.fori_loop(0, crow, patch, 0, unroll=8)
        for cp in store(i):
            cp.start()

    ahead = 2
    for i in range(ahead):
        update(i)

    slot_id = lax.broadcasted_iota(jnp.int32, (blk, rep * crow), 0)
    lane_b = lax.broadcasted_iota(jnp.int32, (1, heads * crow), 1) % crow
    low = lax.broadcasted_iota(jnp.int32, (heads, blk), 0) < rep
    scale = dim ** -0.5
    ms, ls = [], []

    for i in range(nchunk):
        if i + ahead < nchunk:
            update(i + ahead)
        b0 = i * crow
        qt = jnp.concatenate([qbuf[h, b0:b0 + crow, :] for h in range(heads)], axis=0).T
        limit = jnp.zeros((1, heads * crow), jnp.int32)
        for r in range(crow):
            limit = jnp.where(lane_b == r, lens[b0 + r] - base, limit)
        rhs = [jnp.concatenate([jnp.where(lane_b[:, :rep * crow] == r, qt[:, gi * rep * crow:(gi + 1) * rep * crow], 0.0).astype(BF16) for r in range(crow)], axis=0) for gi in range(groups)]
        sts = [dot32(jnp.concatenate([kbuf[b0 + r, gi] for r in range(crow)], axis=1), rhs[gi]) for gi in range(groups)]
        mrow, lrow = [], []
        for gi in range(groups):
            lanes = slice(gi * rep * crow, (gi + 1) * rep * crow)
            s = sts[gi] * scale
            valid = slot_id <= limit[:, lanes]
            s = jnp.where(valid, s, MASK_VALUE)
            m = jnp.max(s, axis=0, keepdims=True)
            p = jnp.where(valid, jnp.exp(s - m), 0.0)
            mrow.append(m)
            lrow.append(jnp.sum(p, axis=0, keepdims=True))
            pbuf[gi * rep * crow:(gi + 1) * rep * crow, :] = p.T
        ms.append(mrow)
        ls.append(lrow)
        for r in range(0, crow, 2):
            lhs = []
            for q in range(2):
                ps = pbuf[pl.ds(r + q, heads, stride=crow), :]
                lhs.append(jnp.concatenate([jnp.where(low, ps, 0.0), jnp.where(low, 0.0, ps)], axis=1))
            vals = jnp.concatenate([vbuf[b0 + r].reshape(groups * blk, dim), vbuf[b0 + r + 1].reshape(groups * blk, dim)], axis=1)
            mix = dot32(jnp.concatenate(lhs, axis=0).astype(BF16), vals)
            o_out[pl.ds(b0 + r, heads, stride=rows), :] = mix[:heads, :dim]
            o_out[pl.ds(b0 + r + 1, heads, stride=rows), :] = mix[heads:, dim:]

    half = heads // CORES
    for ci in range(CORES):
        for h in range(half):
            gi, ri = divmod(ci * half + h, rep)
            lanes = slice(ri * crow, (ri + 1) * crow)
            st_out[ci, h:h + 1, :] = jnp.concatenate([mrow[gi][:, lanes] for mrow in ms], axis=1)
            st_out[ci, half + h:half + h + 1, :] = jnp.concatenate([lrow[gi][:, lanes] for lrow in ls], axis=1)

    def drain(i, _):
        for cp in store(i):
            cp.wait()
        return 0

    lax.fori_loop(0, nchunk, drain, 0)


def attention(hidden, seq_lens, k_cache, v_cache, gain, w_q, w_k, w_v):
    rows, groups, blk, dim = k_cache.shape
    heads = w_q.shape[1] // dim
    width = w_q.shape[0]
    nw = (w_q.shape[1] + w_k.shape[1] + w_v.shape[1]) // COLS
    nchunk = 4
    any_spec = pl.BlockSpec(memory_space=pl.ANY)
    vm = pl.BlockSpec(memory_space=pltpu.VMEM)
    return pl.pallas_call(
        attn_kernel,
        name='block_attention',
        out_shape=(pltpu.VMEM((heads * rows, dim), F32),
                   pltpu.VMEM((CORES, heads, rows), F32),
                   jax.ShapeDtypeStruct(k_cache.shape, BF16),
                   jax.ShapeDtypeStruct(v_cache.shape, BF16)),
        in_specs=[any_spec] * 8,
        out_specs=(vm, vm, any_spec, any_spec),
        scratch_shapes=[
            pltpu.SMEM((rows,), jnp.int32),
            pltpu.VMEM((rows, width), BF16),
            pltpu.VMEM((width // LANES, LANES), BF16),
            pltpu.VMEM((rows, width), BF16),
            pltpu.VMEM((nw, width, COLS), BF16),
            pltpu.VMEM((heads, rows, dim), F32),
            pltpu.VMEM((groups, rows, dim), F32),
            pltpu.VMEM((groups, rows, dim), F32),
            pltpu.VMEM(k_cache.shape, BF16),
            pltpu.VMEM(v_cache.shape, BF16),
            pltpu.VMEM((heads * rows // nchunk, blk), F32),
            pltpu.SemaphoreType.DMA((4,)),
            pltpu.SemaphoreType.DMA((nw,)),
            pltpu.SemaphoreType.DMA((nchunk,)),
            pltpu.SemaphoreType.DMA((nchunk,)),
            pltpu.SemaphoreType.DMA((nchunk,)),
            pltpu.SemaphoreType.DMA((nchunk,)),
        ],
        compiler_params=pltpu.CompilerParams(vmem_limit_bytes=VMEM_LIMIT),
    )(seq_lens, hidden, gain.reshape(width // LANES, LANES), w_q, w_k, w_v, k_cache, v_cache)


def mlp_kernel(nx, ny, hid, o_b, st_b, gain, wo, wg, wu, wd, out,
               wo_b, wg_b, wu_b, wd_b, hid_b, gain_b, gf_b, po_b, pst_b, oc_b, cst_b, xo_b, xst_b, tst_b,
               att_b, pw_b, rw_b, mid_b, ss_b, g_acc, u_acc, act_b, ab_b, pd_b, rd_b, fin_b,
               lsem, osem, gsem, usem, dsem, ds_s, ds_r, xs_s, xs_r, as_s, as_r, ws_s, ws_r, ms_s, ms_r, cs_s, ss_s, ss_r,
               dn_s, dn_r, fs_s, fs_r, fp_s, fp_r):
    sp = lax.axis_index('sp')
    y = lax.axis_index('tp')
    x = sp // CORES
    c = sp % CORES
    oc = 1 - c
    half_h, rows, dim = po_b.shape
    xr = rows // nx
    width = gain.shape[0] * LANES
    hw = width // CORES
    cw = hw // ny
    nq, qw = mid_b.shape[2], mid_b.shape[4]
    partner = {'tp': y, 'sp': x * CORES + oc}
    far = [2, 1, 3] if ny == 4 else list(range(1, ny))
    near = [1, 3, 2] if ny == 4 else list(range(1, ny))

    def peer(yy, xx):
        return {'tp': yy, 'sp': xx * CORES + c}

    def cross(yy):
        return {'tp': yy, 'sp': x * CORES + oc}

    def rcopy(src, dst, ssem, rsem, dev):
        return pltpu.make_async_remote_copy(src_ref=src, dst_ref=dst, send_sem=ssem, recv_sem=rsem, device_id=dev, device_id_type=MESH)

    def cols(i, n):
        return pl.ds(pl.multiple_of(i * n, n), n)

    loads = [
        pltpu.make_async_copy(hid.at[pl.ds(x * xr, xr), pl.ds(pl.multiple_of(c * hw + y * cw, cw), cw)], hid_b, lsem.at[2]),
        pltpu.make_async_copy(gain, gain_b, lsem.at[3]),
    ]
    for cp in loads:
        cp.start()
    steps = wg_b.shape[0]
    inner = steps * COLS

    def row_load(w, w_b, sem, n, j):
        r = cols(j, w_b.shape[0] // n)
        return pltpu.make_async_copy(w.at[r, cols(c, hw)], w_b.at[r], sem.at[j])

    def col_loads(j):
        r = cols(c * steps + j, COLS)
        return (pltpu.make_async_copy(wg.at[:, r], wg_b.at[j], gsem.at[j]), pltpu.make_async_copy(wu.at[:, r], wu_b.at[j], usem.at[j]))

    wo_loads = [row_load(wo, wo_b, osem, osem.shape[0], j) for j in range(osem.shape[0])]
    wd_loads = [row_load(wd, wd_b, dsem, steps, j) for j in range(steps)]
    gu_plan = [range(0, 3), range(3, 5), range(5, steps)]
    wd_plan = [range(0, 4), range(4, steps)]

    def fetch_gu(stage):
        for j in gu_plan[stage]:
            for cp in col_loads(j):
                cp.start(priority=1)

    def fetch_wd(stage):
        for j in wd_plan[stage]:
            wd_loads[j].start(priority=1)

    for cp in wo_loads:
        cp.start(priority=1)
    fetch_gu(0)

    barrier = pltpu.get_barrier_semaphore()
    pl.semaphore_signal(barrier, inc=1, device_id=partner, device_id_type=MESH)
    for k in range(1, nx):
        pl.semaphore_signal(barrier, inc=1, device_id=peer(y, (x + k) % nx), device_id_type=MESH)
    for k in range(1, ny):
        pl.semaphore_signal(barrier, inc=1, device_id=peer((y + k) % ny, x), device_id_type=MESH)
        pl.semaphore_signal(barrier, inc=1, device_id=cross((y + k) % ny), device_id_type=MESH)
    pl.semaphore_wait(barrier, 1 + (nx - 1) + 2 * (ny - 1))

    def head_rows(h):
        return pl.ds(pl.multiple_of(h * rows, rows), rows)

    swap = [rcopy(st_b.at[oc], pst_b, ds_s.at[half_h], ds_r.at[half_h], partner)]
    for h in range(half_h):
        swap.append(rcopy(o_b.at[head_rows(half_h * oc + h)], po_b.at[h], ds_s.at[h], ds_r.at[h], partner))
    for cp in swap:
        cp.start()
    fetch_gu(1)
    swap[0].wait_recv()
    s0 = st_b[c]
    s1 = pst_b[...]
    m0, l0, m1, l1 = s0[:half_h], s0[half_h:], s1[:half_h], s1[half_h:]
    mm = jnp.maximum(m0, m1)
    a0, a1 = jnp.exp(m0 - mm), jnp.exp(m1 - mm)
    cst_b[...] = jnp.concatenate([mm, a0 * l0 + a1 * l1], axis=0)

    far_x = [2, 1, 3] if nx == 4 else list(range(1, nx))
    sends = []
    for k in far_x:
        sends.append(rcopy(cst_b, xst_b.at[x], xs_s.at[k - 1, half_h], xs_r.at[x, half_h], peer(y, (x + k) % nx)))
    for cp in sends:
        cp.start()
    tr = jnp.concatenate([a0, a1], axis=0).T
    for h in range(half_h):
        swap[1 + h].wait_recv()
        oc_b[h] = o_b[head_rows(half_h * c + h), :] * tr[:, h:h + 1] + po_b[h] * tr[:, half_h + h:half_h + h + 1]
        for k in far_x:
            xx = (x + k) % nx
            cp = rcopy(oc_b.at[h, pl.ds(xx * xr, xr), :], xo_b.at[x, h], xs_s.at[k - 1, h], xs_r.at[x, h], peer(y, xx))
            cp.start()
            sends.append(cp)
    fetch_gu(2)
    tst_b[0] = cst_b[...].T
    for k in range(1, nx):
        xx = (x + k) % nx
        rcopy(cst_b, xst_b.at[xx], xs_s.at[k - 1, half_h], xs_r.at[xx, half_h], peer(y, xx)).wait_recv()
        tst_b[k] = xst_b[xx].T
    stats = [tst_b[k, pl.ds(x * xr, xr), :] for k in range(nx)]
    mm = stats[0][:, :half_h]
    for k in range(1, nx):
        mm = jnp.maximum(mm, stats[k][:, :half_h])
    alphas = [jnp.exp(st[:, :half_h] - mm) for st in stats]
    total = alphas[0] * stats[0][:, half_h:]
    for k in range(1, nx):
        total = total + alphas[k] * stats[k][:, half_h:]
    for h in range(half_h):
        acc = oc_b[h, pl.ds(x * xr, xr), :] * alphas[0][:, h:h + 1]
        for k in range(1, nx):
            xx = (x + k) % nx
            rcopy(oc_b.at[h, pl.ds(xx * xr, xr), :], xo_b.at[xx, h], xs_s.at[k - 1, h], xs_r.at[xx, h], peer(y, xx)).wait_recv()
            acc = acc + xo_b[xx, h] * alphas[k][:, h:h + 1]
        att_b[c, h] = (acc / total[:, h:h + 1]).astype(BF16).astype(F32)
        cp = rcopy(att_b.at[c, h], att_b.at[c, h], as_s.at[h], as_r.at[h], partner)
        cp.start()
        sends.append(cp)

    def unit(yy, q):
        return pl.ds(pl.multiple_of(yy * cw + q * qw, qw), qw)

    def send_unit(send_b, recv_b, s_sem, r_sem, q, k):
        yy = (y + k) % ny
        cp = rcopy(send_b.at[q, yy], recv_b.at[q, y], s_sem.at[q, k], r_sem.at[q, y], peer(yy, x))
        cp.start()
        return cp

    def collect(send_b, recv_b, s_sem, r_sem, q):
        total = send_b[q, y]
        for k in range(1, ny):
            yy = (y + k) % ny
            rcopy(send_b.at[q, yy], recv_b.at[q, yy], s_sem.at[q, k], r_sem.at[q, yy], peer(yy, x)).wait_recv()
            total = total + recv_b[q, yy]
        return total

    for cp in loads:
        cp.wait()
    gf_b[...] = gain_b[...].astype(F32)

    for cp in wo_loads:
        cp.wait()
    started = swap + sends

    def attended(ci):
        return jnp.concatenate([att_b[ci, h] for h in range(half_h)], axis=1).astype(BF16)

    own_att = attended(c)
    for q in range(nq):
        for k in far + [0]:
            yy = (y + k) % ny
            pw_b[q, yy] = dot32(own_att, wo_b[cols(c, half_h * dim), unit(yy, q)])
    for h in range(half_h):
        rcopy(att_b.at[oc, h], att_b.at[oc, h], as_s.at[h], as_r.at[h], partner).wait_recv()
    other_att = attended(oc)
    for q in range(nq):
        for k in far + [0]:
            yy = (y + k) % ny
            pw_b[q, yy] = pw_b[q, yy] + dot32(other_att, wo_b[cols(oc, half_h * dim), unit(yy, q)])
            if k:
                started.append(send_unit(pw_b, rw_b, ws_s, ws_r, q, k))
    fetch_wd(0)

    def mid_copy(ci, yy, q, ssem, dev):
        return rcopy(mid_b.at[ci, yy, q], mid_b.at[ci, yy, q], ssem, ms_r.at[ci, yy, q], dev)

    sq = jnp.zeros((xr, 1), F32)
    for q in range(nq):
        piece = (hid_b[:, q * qw:(q + 1) * qw].astype(F32) + collect(pw_b, rw_b, ws_s, ws_r, q)).astype(BF16).astype(F32)
        mid_b[c, y, q] = piece
        sq = sq + jnp.sum(piece * piece, axis=-1, keepdims=True)
        sends = []
        if q == nq - 1:
            wide = jnp.broadcast_to(sq, (xr, LANES))
            ss_b[c, y] = jnp.concatenate([wide] * (LANES // xr), axis=0).T[:ss_b.shape[2]]
            sends.append(rcopy(ss_b.at[c, y], ss_b.at[c, y], ss_s.at[0, 0], ss_r.at[c, y], partner))
            for k in range(1, ny):
                yy = (y + k) % ny
                sends.append(rcopy(ss_b.at[c, y], ss_b.at[c, y], ss_s.at[0, k], ss_r.at[c, y], peer(yy, x)))
                sends.append(rcopy(ss_b.at[c, y], ss_b.at[c, y], ss_s.at[1, k], ss_r.at[c, y], cross(yy)))
        sends.append(mid_copy(c, y, q, cs_s.at[q, 0], partner))
        for k in near:
            sends.append(mid_copy(c, y, q, ms_s.at[q, k], peer((y + k) % ny, x)))
        for cp in sends:
            cp.start()
        started += sends
    fetch_wd(1)

    def ss_wait(ci, yy):
        rcopy(ss_b.at[ci, yy], ss_b.at[ci, yy], ss_s.at[0, 0], ss_r.at[ci, yy], partner).wait_recv()

    ss_wait(oc, y)
    for k in range(1, ny):
        ss_wait(c, (y + k) % ny)
        ss_wait(oc, (y + k) % ny)
    tot = ss_b[0, 0]
    for t in range(1, CORES * ny):
        tot = tot + ss_b[t // ny, t % ny]
    inv = lax.rsqrt(tot.T[:xr, :1] / width + NORM_EPS)
    inv = jnp.broadcast_to(inv, (xr, LANES))

    for j in range(steps):
        for cp in col_loads(j):
            cp.wait()

    def accumulate(ci, yy, first):
        start = ci * hw + yy * cw
        parts = []
        for q in range(nq):
            for j in range(qw // LANES):
                g = gf_b[pl.ds(start // LANES + q * (qw // LANES) + j, 1), :]
                parts.append((mid_b[ci, yy, q, :, j * LANES:(j + 1) * LANES] * inv * g).astype(BF16))
        u = jnp.concatenate(parts, axis=1)
        r = pl.ds(pl.multiple_of(start, cw), cw)
        for j in range(steps):
            gp = dot32(u, wg_b[j, r, :])
            up = dot32(u, wu_b[j, r, :])
            g_acc[j] = gp if first else g_acc[j] + gp
            u_acc[j] = up if first else u_acc[j] + up

    def other(yy):
        for q in range(nq):
            mid_copy(oc, yy, q, cs_s.at[q, 0], partner).wait_recv()

    accumulate(c, y, True)
    other(y)
    accumulate(oc, y, False)

    def gather_step(i, _):
        k = i + (i // 2) * (1 - 2 * (i % 2)) if ny == 4 else i
        yy = (y + k) % ny
        for q in range(nq):
            mid_copy(c, yy, q, ms_s.at[q, 0], partner).wait_recv()
            mid_copy(c, yy, q, cs_s.at[q, k], partner).start()
        accumulate(c, yy, False)
        other(yy)
        accumulate(oc, yy, False)
        return 0

    lax.fori_loop(1, ny, gather_step, 0)
    for k in range(1, ny):
        for q in range(nq):
            mid_copy(c, (y + k) % ny, q, cs_s.at[q, k], partner).wait_send()

    acts = []
    for j in range(steps):
        gp = g_acc[j]
        act = (gp * jax.nn.sigmoid(gp) * u_acc[j]).astype(BF16)
        ab_b[c, :, j * COLS:(j + 1) * COLS] = act
        act_b[c, j] = act.astype(F32)
        cp = rcopy(act_b.at[c, j], act_b.at[c, j], dn_s.at[j], dn_r.at[j], partner)
        cp.start()
        acts.append(cp)
    for cp in started:
        cp.wait_send()

    for cp in wd_loads:
        cp.wait()

    def down(ci, yy, q):
        return dot32(ab_b[ci], wd_b[cols(ci, inner), unit(yy, q)])

    started = []
    for k in far + [0]:
        yy = (y + k) % ny
        pd_b[0, yy] = down(c, yy, 0)
    for j in range(steps):
        rcopy(act_b.at[oc, j], act_b.at[oc, j], dn_s.at[j], dn_r.at[j], partner).wait_recv()
        ab_b[oc, :, j * COLS:(j + 1) * COLS] = act_b[oc, j].astype(BF16)
    for q in range(nq):
        for k in far + [0]:
            yy = (y + k) % ny
            rest = down(oc, yy, q)
            pd_b[q, yy] = (pd_b[q, yy] if q == 0 else down(c, yy, q)) + rest
            if k:
                started.append(send_unit(pd_b, rd_b, fs_s, fs_r, q, k))

    def slot(yy, xx, q):
        return fin_b.at[xx, yy, c, q]

    def place(k1, k2, ci):
        oi = 1 - ci
        return (y + k1 * oi + k2 * ci) % ny, (x + k1 * ci + k2 * oi) % nx

    def fcopy(yy, xx, q, ssem, dev):
        return rcopy(slot(yy, xx, q), slot(yy, xx, q), ssem, fp_r.at[xx, yy, c, q], dev)

    def spread(k1, q):
        sy, sx = place(k1, 0, c)
        for k2 in far_x:
            ty, tx = place(0, k2, c)
            cp = fcopy(sy, sx, q, fp_s.at[q, k1, k2], peer(ty, tx))
            cp.start()
            started.append(cp)
        cp = fcopy(sy, sx, q, fp_s.at[q, k1, 0], partner)
        cp.start()
        started.append(cp)

    def landed(yy, xx, ci, q):
        rcopy(fin_b.at[xx, yy, ci, q], fin_b.at[xx, yy, ci, q], fp_s.at[0, 0, 0], fp_r.at[xx, yy, ci, q], partner).wait_recv()

    def emit(yy, xx, ci, q):
        r = pl.ds(pl.multiple_of(xx * xr, xr), xr)
        out[r, pl.ds(pl.multiple_of(ci * hw + yy * cw + q * qw, qw), qw)] = fin_b[xx, yy, ci, q].astype(BF16)

    for q in range(nq):
        fin_b[x, y, c, q] = (mid_b[c, y, q] + collect(pd_b, rd_b, fs_s, fs_r, q)).astype(BF16).astype(F32)
        for k1 in far:
            ty, tx = place(k1, 0, c)
            cp = fcopy(y, x, q, fp_s.at[q, 0, nx + k1], peer(ty, tx))
            cp.start()
            started.append(cp)
        spread(0, q)
    for q in range(nq):
        for k1 in near:
            sy, sx = place(k1, 0, c)
            landed(sy, sx, c, q)
            spread(k1, q)
        emit(y, x, c, q)
        for k1 in near:
            emit(*place(k1, 0, c), c, q)
    order = [(k1, k2) for k1 in [0] + near for k2 in near]
    for q in range(nq):
        for k1, k2 in order:
            sy, sx = place(k1, k2, c)
            landed(sy, sx, c, q)
            cp = fcopy(sy, sx, q, fp_s.at[q, k1, nx + ny + k2], partner)
            cp.start()
            started.append(cp)
            emit(sy, sx, c, q)
    for q in range(nq):
        for k1, k2 in [(k1, 0) for k1 in [0] + near] + order:
            sy, sx = place(k1, k2, oc)
            landed(sy, sx, oc, q)
            emit(sy, sx, oc, q)
    for cp in acts + started:
        cp.wait_send()


def mlp(mesh, hidden, o_part, stats, gain, w_o, w_gate, w_up, w_down):
    rows, width = hidden.shape
    heads = stats.shape[1]
    dim = o_part.shape[1]
    half_h = heads // CORES
    nx = mesh.shape['sp'] // CORES
    ny = mesh.shape['tp']
    xr = rows // nx
    hw = width // CORES
    cw = hw // ny
    inner = w_gate.shape[1] // CORES
    nq = cw // QCOLS
    steps = inner // COLS
    any_spec = pl.BlockSpec(memory_space=pl.ANY)
    vm = pl.BlockSpec(memory_space=pltpu.VMEM)
    dma = pltpu.SemaphoreType.DMA
    return pl.pallas_call(
        functools.partial(mlp_kernel, nx, ny),
        name='exchange_mlp',
        out_shape=pltpu.VMEM(hidden.shape, BF16),
        in_specs=[any_spec, vm, vm] + [any_spec] * 5,
        out_specs=vm,
        scratch_shapes=[
            pltpu.VMEM((w_o.shape[0], hw), BF16),
            pltpu.VMEM((steps, width, COLS), BF16),
            pltpu.VMEM((steps, width, COLS), BF16),
            pltpu.VMEM((w_down.shape[0], hw), BF16),
            pltpu.VMEM((xr, cw), BF16),
            pltpu.VMEM((width // LANES, LANES), BF16),
            pltpu.VMEM((width // LANES, LANES), F32),
            pltpu.VMEM((half_h, rows, dim), F32),
            pltpu.VMEM((heads, rows), F32),
            pltpu.VMEM((half_h, rows, dim), F32),
            pltpu.VMEM((heads, rows), F32),
            pltpu.VMEM((nx, half_h, xr, dim), F32),
            pltpu.VMEM((nx, heads, rows), F32),
            pltpu.VMEM((nx, rows, heads), F32),
            pltpu.VMEM((CORES, half_h, xr, dim), F32),
            pltpu.VMEM((nq, ny, xr, QCOLS), F32),
            pltpu.VMEM((nq, ny, xr, QCOLS), F32),
            pltpu.VMEM((CORES, ny, nq, xr, QCOLS), F32),
            pltpu.VMEM((CORES, ny, 8, LANES), F32),
            pltpu.VMEM((steps, xr, COLS), F32),
            pltpu.VMEM((steps, xr, COLS), F32),
            pltpu.VMEM((CORES, steps, xr, COLS), F32),
            pltpu.VMEM((CORES, xr, inner), BF16),
            pltpu.VMEM((nq, ny, xr, QCOLS), F32),
            pltpu.VMEM((nq, ny, xr, QCOLS), F32),
            pltpu.VMEM((nx, ny, CORES, nq, xr, QCOLS), F32),
            dma((4,)), dma((4,)), dma((steps,)), dma((steps,)), dma((steps,)),
            dma((half_h + 1,)), dma((half_h + 1,)),
            dma((nx, half_h + 1)), dma((nx, half_h + 1)),
            dma((half_h,)), dma((half_h,)),
            dma((nq, ny)), dma((nq, ny)),
            dma((nq, ny)), dma((CORES, ny, nq)), dma((nq, ny)),
            dma((CORES, ny)), dma((CORES, ny)),
            dma((steps,)), dma((steps,)),
            dma((nq, ny)), dma((nq, ny)),
            dma((nq, ny, 2 * nx + ny)), dma((nx, ny, CORES, nq)),
        ],
        compiler_params=pltpu.CompilerParams(vmem_limit_bytes=VMEM_LIMIT, collective_id=0, has_side_effects=True),
    )(hidden, pltpu.with_memory_space_constraint(o_part, pltpu.VMEM), pltpu.with_memory_space_constraint(stats, pltpu.VMEM), gain.reshape(width // LANES, LANES), w_o, w_gate, w_up, w_down)


def solution(mesh):
    cache_spec = P('dp', 'tp', 'sp', None)
    row_spec = P('dp', None)
    col_spec = P(None, 'tp')
    inner_spec = P('tp', None)
    gain_spec = P(None)

    def local_step(hidden, seq_lens, k_cache, v_cache, attn_norm, w_q, w_k, w_v, w_o, mlp_norm, w_gate, w_up, w_down):
        o_part, stats, k_out, v_out = attention(hidden, seq_lens, k_cache, v_cache, attn_norm, w_q, w_k, w_v)
        hidden_out = mlp(mesh, hidden, o_part, stats, mlp_norm, w_o, w_gate, w_up, w_down)
        return hidden_out, k_out, v_out

    return jax.shard_map(local_step, mesh=mesh, in_specs=(row_spec, P('dp'), cache_spec, cache_spec, gain_spec, col_spec, col_spec, col_spec, inner_spec, gain_spec, col_spec, col_spec, inner_spec), out_specs=(row_spec, cache_spec, cache_spec), check_vma=False)
```
